512 devices in a mesh: frame: 16 (over z_hi, x), tile: 32 (over y, z_lo, core).
Axes of the slice: x: 4, y: 8, z: 8 (z_hi: 4, z_lo: 2; z = z_hi * 2 + z_lo), core: 2. Of those that a mesh axis runs over, the one named last changes fastest.
Arguments:
- saved_codes: bfloat16 [32, 128, 32, 128], P('frame', 'tile'), may hold values from -1 to 1
- saved_scales: float32 [32, 128, 32], P('frame', 'tile'), may hold values from 0.5 to 2.5
- kernels: bfloat16 [2, 27, 128, 128], replicated, may hold values from -0.109375 to 0.109375
- norm_gains: float32 [2, 128], replicated, may hold values from 0.25 to 1.75
- cotangent: bfloat16 [32, 128, 32, 128], P('frame', 'tile'), may hold values from -13 to 13
Outputs:
- input_grad: bfloat16 [32, 128, 32, 128], P('frame', 'tile')
- kernel_grads: float32 [54, 128, 128], P(None, 'tile', 'frame')
The draws below stay inside these ranges and needn't reach their ends.
All inputs are finite; a program needn't handle non-finite values.
Results may differ from the reference program's by a relative error of at most 0.028.
Values may be sent and summed in bfloat16 or wider, within the bound.
No kernel may reach another device: no remote copies, remote signals or barrier semaphores. Data moves between devices by JAX's collectives and lax.ppermute only.
A program may use at most 64 MiB of HBM per device.

```python
import math
import jax
import jax.numpy as jnp
from jax import lax

C = 128
LAYERS = 2
W = 32
NT = 32
NH = 128


def draw_cotangent(key, part):
    first = jax.random.fold_in(key, 0)
    frame_rise = 0.5 + 1.5 * jnp.arange(NT, dtype=jnp.float32) / NT
    row_rise = 0.6 + 1.2 * jnp.arange(NH, dtype=jnp.float32) / NH
    scale = frame_rise[:, None, None, None] * row_rise[None, :, None, None]
    base = jnp.clip(jax.random.normal(first, (NT, NH, W, C), jnp.float32), -3.5, 3.5)
    return (base * scale).astype(jnp.bfloat16)


def shard_levels(key, shape, pieces, least, high):
    factor_of, own = 1.0, jax.random.fold_in(key, 6)
    for position, shards_of in pieces:
        heights = jnp.exp(jax.random.uniform(jax.random.fold_in(own, position), (shards_of,), jnp.float32, least / len(pieces), high / len(pieces)))
        factor_of = factor_of * jnp.repeat(heights, shape[position] // shards_of).reshape([-1 if axis == position else 1 for axis in range(len(shape))])
    return factor_of


def noise(rng, shape, scale, reach, kind=jnp.bfloat16):
    return jnp.clip(scale * jax.random.normal(rng, shape, jnp.float32), -reach, reach).astype(kind)


def setup_inputs(seed: int = 0) -> dict:
    key_of = jax.random.split(jax.random.key(seed), 6)
    return {
        "saved_codes": jnp.clip(jax.random.uniform(key_of[0], (NT, NH, W, C), jnp.float32, -1.0, 1.0) * shard_levels(key_of[0], (NT, NH, W, C), ((0, 16), (1, 32)), -0.4, 0.0), -1.0, 1.0).astype(jnp.bfloat16),
        "saved_scales": jnp.clip(jnp.exp(math.log(2.5) - 1.609438 * jax.random.uniform(key_of[1], (NT, NH, W), jnp.float32) ** shard_levels(key_of[1], (NT, NH, W), ((0, 16), (1, 32)), -0.2, 0.2)), 0.5, 2.5),
        "kernels": noise(key_of[2], (LAYERS, 27, C, C), (27 * C) ** -0.5, 0.109375),
        "norm_gains": jnp.clip(1.0 + 0.15 * jax.random.normal(key_of[3], (LAYERS, C), jnp.float32), 0.25, 1.75),
        "cotangent": draw_cotangent(jax.random.fold_in(key_of[5], 71), 0),
    }


EPS = 1e-06

def convolve(inputs, weights):
    channels = weights.shape[-1]
    kernel = weights.reshape(3, 3, 3, channels, channels)
    result = lax.conv_general_dilated(inputs[None], kernel, (1, 1, 1), ((2, 0), (1, 1), (1, 1)), dimension_numbers=('NDHWC', 'DHWIO', 'NDHWC'), precision=lax.Precision.HIGHEST)
    return result[0]

def reference(saved_codes, saved_scales, kernels, norm_gains, cotangent):
    layer_in = (saved_codes.astype(jnp.float32) * saved_scales[..., None]).astype(jnp.bfloat16)
    inputs_list = []
    states = []
    for layer in range(LAYERS):
        inputs_list.append(layer_in)
        pre_norm = convolve(layer_in.astype(jnp.float32), kernels[layer].astype(jnp.float32))
        inverse = lax.rsqrt(lax.optimization_barrier(jnp.mean(pre_norm * pre_norm, axis=-1, keepdims=True)) + EPS)
        normed = pre_norm * inverse * norm_gains[layer]
        states.append((pre_norm, inverse, normed))
        layer_in = jax.nn.silu(normed).astype(jnp.bfloat16)
    upstream = cotangent
    grads_list = [None] * LAYERS
    for layer in reversed(range(LAYERS)):
        pre_norm, inverse, normed = states[layer]
        sigma = jax.nn.sigmoid(normed)
        scaled = norm_gains[layer] * upstream.astype(jnp.float32) * sigma * (1.0 + normed * (1.0 - sigma))
        mixed = lax.optimization_barrier(jnp.mean(pre_norm * scaled, axis=-1, keepdims=True))
        pre_grad = (inverse * scaled - pre_norm * inverse ** 3 * mixed).astype(jnp.bfloat16)
        pre_grad = lax.optimization_barrier(pre_grad).astype(jnp.float32)
        _, pullback = jax.vjp(convolve, inputs_list[layer].astype(jnp.float32), kernels[layer].astype(jnp.float32))
        input_part, kernel_part = pullback(pre_grad)
        grads_list[layer] = kernel_part
        upstream = input_part.astype(jnp.bfloat16)
    total_cells = NT * NH * W
    kernel_grads = jnp.stack(grads_list).reshape(LAYERS * 27, C, C) / jnp.sqrt(jnp.float32(total_cells))
    return (upstream, kernel_grads)
```

```python
import math

import jax
import jax.numpy as jnp
from jax import lax
from jax.experimental import pallas as pl
from jax.experimental.pallas import tpu as pltpu
from jax.sharding import PartitionSpec as P

EPS = 1e-06


def with_halo(cells, sides, width):
    for axis, dim in sides:
        count = lax.axis_size(axis)
        ends = count - 1
        head = lax.slice_in_dim(cells, 0, width, axis=dim)
        tail = lax.slice_in_dim(cells, cells.shape[dim] - width, cells.shape[dim], axis=dim)
        cells = jnp.concatenate(
            [
                lax.ppermute(tail, axis, [(i, (i + 1) % count) for i in range(ends)]),
                cells,
                lax.ppermute(head, axis, [((i + 1) % count, i) for i in range(ends)]),
            ],
            axis=dim,
        )
    return cells


def from_behind(value, axis, steps):
    count = lax.axis_size(axis)
    first, last = (max(0, -steps), min(count, count - steps))
    return lax.ppermute(value, axis, [(source, source + steps) for source in range(first, last)])


def parts_kernel(first_ref, second_ref, *part_refs):
    taps = first_ref.shape[0]
    for index, part_ref in enumerate(part_refs):
        tap, half = divmod(index, 2)
        source = first_ref if tap < taps else second_ref
        rows = source.shape[1] // 2
        block = source[tap % taps, half * rows : (half + 1) * rows]
        part_ref[...] = block.reshape(part_ref.shape).astype(part_ref.dtype)


def in_parts(first, second, pieces):
    taps, rows, lanes = first.shape
    shape = jax.ShapeDtypeStruct((pieces // 2, rows // pieces, lanes), jnp.bfloat16)
    return pl.pallas_call(parts_kernel, out_shape=[shape] * (4 * taps))(first, second)


def pick_kernel(scale, *refs):
    *part_refs, out_ref, rows_ref = refs
    position = lax.axis_index("tile")
    blocks = part_refs[0].shape[0]
    width = out_ref.shape[-1]
    upper = position >= blocks
    index = jnp.where(upper, position - blocks, position)
    for tap in range(len(part_refs) // 2):
        low = part_refs[2 * tap][index].astype(jnp.float32)
        high = part_refs[2 * tap + 1][index].astype(jnp.float32)
        rows_ref[tap] = jnp.where(upper, high, low) * scale
    lanes = rows_ref.shape[-1]
    shift = lanes - lax.axis_index("frame") * width
    out_ref[...] = pltpu.roll(rows_ref[...], shift, 2)[:, :, :width]


def picked(parts, width, scale):
    taps = len(parts) // 2
    _, rows, lanes = parts[0].shape
    return pl.pallas_call(
        lambda *refs: pick_kernel(scale, *refs),
        out_shape=jax.ShapeDtypeStruct((taps, rows, width), jnp.float32),
        scratch_shapes=[pltpu.VMEM((taps, rows, lanes), jnp.float32)],
    )(*parts)


def patches(extended, frames, rows, columns, offset, sign):
    pieces = []
    for depth in range(3):
        for down in range(3):
            for across in range(3):
                first_frame = offset + sign * depth
                first_row = 1 + sign * (down - 1) + (offset - 2 * (sign < 0) * 0) * 0
                first_col = 1 + sign * (across - 1)
                pieces.append(
                    extended[
                        first_frame : first_frame + frames,
                        first_row : first_row + rows,
                        first_col : first_col + columns,
                    ]
                )
    joined = jnp.concatenate(pieces, axis=-1)
    return joined.reshape(frames * rows * columns, joined.shape[-1])


def pad_columns(block):
    return jnp.pad(block, ((0, 0), (0, 0), (1, 1), (0, 0)))


def extend_input(layer_in):
    own_rows = with_halo(layer_in, (("tile", 1),), 1)
    earlier = from_behind(own_rows, "frame", 1)
    widened = jnp.concatenate([earlier, own_rows], axis=0)
    return pad_columns(widened)


def extend_cotangent(pre_grad):
    later = from_behind(pre_grad, "frame", -1)
    joined = jnp.concatenate([pre_grad, later], axis=0)
    widened = with_halo(joined, (("tile", 1),), 1)
    return pad_columns(widened)


def local(saved_codes, saved_scales, kernels, norm_gains, cotangent):
    frames, rows, columns, channels = saved_codes.shape
    layer_count = kernels.shape[0]
    cells = frames * rows * columns
    layer_in = (saved_codes.astype(jnp.float32) * saved_scales[..., None]).astype(jnp.bfloat16)
    extended_list = []
    states = []
    for layer in range(layer_count):
        extended = extend_input(layer_in)
        extended_list.append(extended)
        columns_in = patches(extended, frames, rows, columns, 0, 1)
        forward_kernel = kernels[layer].reshape(27 * channels, channels)
        pre_norm = jnp.dot(columns_in, forward_kernel, preferred_element_type=jnp.float32)
        inverse = lax.rsqrt(jnp.mean(pre_norm * pre_norm, axis=-1, keepdims=True) + EPS)
        normed = pre_norm * inverse * norm_gains[layer]
        states.append((pre_norm, inverse, normed))
        if layer + 1 < layer_count:
            layer_in = (
                jax.nn.silu(normed).astype(jnp.bfloat16).reshape(frames, rows, columns, channels)
            )
    upstream = cotangent.reshape(cells, channels)
    grads_list = [None] * layer_count
    for layer in reversed(range(layer_count)):
        pre_norm, inverse, normed = states[layer]
        sigma = jax.nn.sigmoid(normed)
        scaled = (
            norm_gains[layer]
            * upstream.astype(jnp.float32)
            * sigma
            * (1.0 + normed * (1.0 - sigma))
        )
        mixed = jnp.mean(pre_norm * scaled, axis=-1, keepdims=True)
        pre_grad = (inverse * scaled - pre_norm * inverse**3 * mixed).astype(jnp.bfloat16)
        columns_in = patches(extended_list[layer], frames, rows, columns, 0, 1)
        kernel_part = lax.dot_general(
            columns_in, pre_grad, (((0,), (0,)), ((), ())), preferred_element_type=jnp.float32
        )
        grads_list[layer] = kernel_part.reshape(27, channels, channels)
        spread_grad = extend_cotangent(pre_grad.reshape(frames, rows, columns, channels))
        columns_back = patches(spread_grad, frames, rows, columns, 2, -1)
        back_kernel = jnp.transpose(kernels[layer], (0, 2, 1)).reshape(27 * channels, channels)
        upstream = jnp.dot(columns_back, back_kernel, preferred_element_type=jnp.float32).astype(
            jnp.bfloat16
        )
    input_grad = upstream.reshape(frames, rows, columns, channels)
    total_cells = cells * lax.axis_size("frame") * lax.axis_size("tile")
    parts = in_parts(grads_list[0], grads_list[1], lax.axis_size("tile"))
    summed = lax.psum(parts, ("frame", "tile"))
    kernel_grads = picked(summed, channels // lax.axis_size("frame"), 1.0 / math.sqrt(total_cells))
    return (input_grad, kernel_grads)


def solution(mesh):
    in_specs = (
        P("frame", "tile", None, None),
        P("frame", "tile", None),
        P(),
        P(),
        P("frame", "tile", None, None),
    )
    out_specs = (P("frame", "tile", None, None), P(None, "tile", "frame"))
    return jax.shard_map(local, mesh=mesh, in_specs=in_specs, out_specs=out_specs, check_vma=False)
```

```python
import math

import jax
import jax.numpy as jnp
from jax import lax
from jax.experimental import pallas as pl
from jax.experimental.pallas import tpu as pltpu
from jax.sharding import PartitionSpec as P

EPS = 1e-06
TAPS = 27
F32 = jnp.float32
BF16 = jnp.bfloat16


def call(kernel, out_shape, *operands, scratch=()):
    return pl.pallas_call(
        kernel,
        out_shape=out_shape,
        scratch_shapes=list(scratch),
        compiler_params=pltpu.CompilerParams(vmem_limit_bytes=48 * 2**20),
    )(*operands)


def shifted_columns(block):
    shape = block.shape
    columns = shape[-2]
    flat = block.astype(F32).reshape(-1, shape[-1])
    column = lax.broadcasted_iota(jnp.int32, flat.shape, 0) % columns
    before = jnp.where(column == 0, 0.0, pltpu.roll(flat, 1, 0))
    after = jnp.where(column == columns - 1, 0.0, pltpu.roll(flat, flat.shape[0] - 1, 0))
    return before.astype(BF16).reshape(shape), block, after.astype(BF16).reshape(shape)


def fill(patches, window, frames, rows, sign, seams):
    columns, channels = window[0][0][0].shape
    for row in range(rows):
        for frame in range(frames):
            first = (row * frames + frame) * columns
            for tap in range(TAPS):
                depth, down, across = tap // 9, tap // 3 % 3, tap % 3
                if sign > 0:
                    source = window[row + down][frame + depth][across]
                else:
                    source = window[row + 2 - down][frame + 2 - depth][2 - across]
                    down = 2 - down
                seam = seams.get((row, down))
                if seam is not None:
                    source = jnp.where(seam, jnp.zeros_like(source), source)
                patches[first : first + columns, tap * channels : (tap + 1) * channels] = source


def window_of(rows):
    return [[shifted_columns(block) for block in row] for row in rows]


def forward_rows(rows, frames, own_ref, earlier_ref):
    return [
        [earlier_ref[row, frame] for frame in range(frames)]
        + [own_ref[row, frame] for frame in range(frames)]
        for row in range(rows)
    ]


def silu_parts(pre_norm, gain):
    inverse = lax.rsqrt(jnp.mean(pre_norm * pre_norm, axis=-1, keepdims=True) + EPS)
    normed = pre_norm * inverse * gain
    return inverse, normed, 1.0 / (1.0 + jnp.exp(-normed))


def pre_norm_gradient(pre_norm, gain, upstream):
    inverse, normed, sigma = silu_parts(pre_norm, gain)
    scaled = gain * upstream * sigma * (1.0 + normed * (1.0 - sigma))
    mixed = jnp.mean(pre_norm * scaled, axis=-1, keepdims=True)
    return (inverse * scaled - pre_norm * inverse**3 * mixed).astype(BF16)


def at_last_tile():
    return lax.axis_index("tile") == lax.axis_size("tile") - 1


def first_rows(own_ref, earlier_ref, below_ref, frames, rows, total):
    result = []
    for row in range(total):
        if row < rows:
            result.append(
                [earlier_ref[frame, row] for frame in range(frames)]
                + [own_ref[frame, row] for frame in range(frames)]
            )
        else:
            result.append(
                [below_ref[frame * rows + row - rows] for frame in range(2 * frames)]
            )
    return result


def first_forward(own_ref, earlier_ref, below_ref, kernel_ref, gain_ref, next_ref, pre_ref, patches):
    frames, rows, columns, channels = own_ref.shape
    last = at_last_tile()
    window = window_of(first_rows(own_ref, earlier_ref, below_ref, frames, rows, 2 * rows))
    fill(patches, window, frames, 2 * rows - 2, 1, {(rows - 2, 2): last, (rows - 1, 0): last})
    pre_norm = jnp.dot(
        patches[...], kernel_ref[...].reshape(TAPS * channels, channels), preferred_element_type=F32
    )
    _, normed, sigma = silu_parts(pre_norm, gain_ref[0:1])
    next_ref[...] = (normed * sigma).astype(BF16).reshape(next_ref.shape)
    pre_ref[...] = pre_norm[: pre_ref.shape[0]]


def second_forward(own_ref, earlier_ref, top_ref, low_ref, kernel_ref, gain_ref, grad_ref, patches):
    total, frames, columns, channels = own_ref.shape
    rows = total - 2
    last = at_last_tile()
    window = window_of(forward_rows(total, frames, own_ref, earlier_ref))
    fill(patches, window, frames, rows, 1, {(rows - 3, 2): last, (rows - 2, 0): last})
    pre_norm = jnp.dot(
        patches[...], kernel_ref[...].reshape(TAPS * channels, channels), preferred_element_type=F32
    )
    spread = []
    for row in range(rows):
        for frame in range(frames):
            if row < rows - 2:
                spread.append(top_ref[frame, row + 2])
            else:
                spread.append(low_ref[frame * 2 + row - rows + 2])
    upstream = jnp.concatenate(spread, axis=0).astype(F32)
    grad_ref[...] = pre_norm_gradient(pre_norm, gain_ref[1:2], upstream).reshape(grad_ref.shape)


def backward_rows(own_ref, later_ref, above_ref, frames):
    rows = own_ref.shape[0]
    result = []
    for row in range(2):
        result.append([above_ref[row, frame] for frame in range(2 * frames)])
    for row in range(rows):
        result.append(
            [own_ref[row, frame] for frame in range(frames)]
            + [later_ref[row, frame] for frame in range(frames)]
        )
    return result


def back_product(patches, kernel_ref):
    turned = jnp.concatenate([kernel_ref[tap] for tap in range(TAPS)], axis=1)
    return lax.dot_general(
        patches[...], turned, (((1,), (1,)), ((), ())), preferred_element_type=F32
    )


def second_backward(
    own_ref, later_ref, above_ref, kernel_ref, gain_ref, pre_ref, grad_ref, patches
):
    rows, frames, columns, channels = own_ref.shape
    last = at_last_tile()
    window = window_of(backward_rows(own_ref, later_ref, above_ref, frames))
    fill(patches, window, frames, rows, -1, {(rows - 2, 2): last, (rows - 1, 0): last})
    upstream = back_product(patches, kernel_ref).astype(BF16).astype(F32)
    grad_ref[...] = pre_norm_gradient(pre_ref[...], gain_ref[0:1], upstream).reshape(grad_ref.shape)


def first_backward(own_ref, later_ref, above_ref, kernel_ref, out_ref, patches):
    rows, frames, columns, channels = own_ref.shape
    first, last = lax.axis_index("tile") == 0, at_last_tile()
    window = window_of(backward_rows(own_ref, later_ref, above_ref, frames))
    fill(patches, window, frames, rows, -1, {(0, 0): first, (rows - 1, 2): last})
    grad = back_product(patches, kernel_ref).astype(BF16)
    for row in range(rows):
        for frame in range(frames):
            cell = (row * frames + frame) * columns
            out_ref[frame, row] = grad[cell : cell + columns]


def split_gradient(patches, grad_ref, keep_ref, send_ref):
    chips, _, share, channels = keep_ref.shape
    odd = lax.axis_index("tile") % 2 == 1
    grad = grad_ref[...].reshape(-1, channels)
    for tap in range(TAPS):
        block = lax.dot_general(
            patches[:, tap * channels : (tap + 1) * channels],
            grad,
            (((0,), (0,)), ((), ())),
            preferred_element_type=F32,
        ).reshape(chips, 2, share, channels)
        even_part, odd_part = block[:, 0], block[:, 1]
        keep_ref[:, tap] = jnp.where(odd, odd_part, even_part).astype(BF16)
        send_ref[:, tap] = jnp.where(odd, even_part, odd_part).astype(BF16)


def second_kernel_gradient(own_ref, earlier_ref, grad_ref, keep_ref, send_ref, patches):
    total, frames, columns, channels = own_ref.shape
    rows = total - 2
    last = at_last_tile()
    window = window_of(forward_rows(total, frames, own_ref, earlier_ref))
    fill(patches, window, frames, rows, 1, {(rows - 3, 2): last, (rows - 2, 0): last})
    split_gradient(patches, grad_ref, keep_ref, send_ref)


def first_kernel_gradient(own_ref, earlier_ref, below_ref, grad_ref, keep_ref, send_ref, patches):
    frames, rows, columns, channels = own_ref.shape
    last = at_last_tile()
    window = window_of(first_rows(own_ref, earlier_ref, below_ref, frames, rows, rows + 2))
    fill(patches, window, frames, rows, 1, {(rows - 2, 2): last, (rows - 1, 0): last})
    split_gradient(patches, grad_ref, keep_ref, send_ref)


def add_pairs(keep_first, came_first, keep_second, came_second, out_ref):
    taps = keep_first.shape[1]
    out_ref[:, :taps] = (keep_first[...].astype(F32) + came_first[...].astype(F32)).astype(BF16)
    out_ref[:, taps:] = (keep_second[...].astype(F32) + came_second[...].astype(F32)).astype(BF16)


def sum_tiles(in_ref, out_ref, rows_ref):
    chips, taps, share, channels = in_ref.shape
    groups, width, _ = out_ref.shape
    total = in_ref[0].astype(F32)
    for chip in range(1, chips):
        total = total + in_ref[chip].astype(F32)
    rows_ref[...] = jnp.zeros_like(rows_ref)
    rows_ref[: taps * share] = total.reshape(taps * share, channels)
    out_ref[...] = rows_ref[...].T.reshape(groups, width, -1).astype(BF16)


def sum_frames(scale, in_ref, out_ref):
    groups = in_ref.shape[0]
    total = in_ref[0].astype(F32)
    for group in range(1, groups):
        total = total + in_ref[group].astype(F32)
    out_ref[...] = total.T[: out_ref.shape[0]] * scale


def shape_of(*dims, dtype=BF16):
    return jax.ShapeDtypeStruct(dims, dtype)


def local(saved_codes, saved_scales, kernels, norm_gains, cotangent):
    frames, rows, columns, channels = saved_codes.shape
    tiles, groups = lax.axis_size("tile"), lax.axis_size("frame")
    cells = frames * rows * columns
    block = (columns, channels)

    def patch_scratch(count):
        return (pltpu.VMEM((count, TAPS * channels), BF16),)

    def next_frames(value):
        return lax.ppermute(value, "frame", [(i, i + 1) for i in range(groups - 1)])

    def earlier_frames(value):
        return lax.ppermute(value, "frame", [(i + 1, i) for i in range(groups - 1)])

    def from_below(value):
        return lax.ppermute(value, "tile", [((i + 1) % tiles, i) for i in range(tiles)])

    def from_above(value):
        return lax.ppermute(value, "tile", [(i, (i + 1) % tiles) for i in range(tiles)])

    def partner(value):
        return lax.ppermute(value, "tile", [(i, i ^ 1) for i in range(tiles)])

    own_0 = (saved_codes.astype(F32) * saved_scales[..., None]).astype(BF16)
    earlier_0 = next_frames(own_0)
    sent = jnp.concatenate(
        [
            earlier_0.reshape(frames * rows, *block),
            own_0.reshape(frames * rows, *block),
            cotangent[:, :2].reshape(frames * 2, *block),
        ],
        axis=0,
    )
    below = from_below(sent)
    below_0, low = below[: 2 * frames * rows], below[2 * frames * rows :]
    wide = 2 * rows - 2
    own_1, pre_0 = call(
        first_forward,
        (shape_of(wide, frames, *block), shape_of(cells, channels, dtype=F32)),
        own_0,
        earlier_0,
        below_0,
        kernels[0],
        norm_gains,
        scratch=patch_scratch(wide * frames * columns),
    )
    earlier_1 = next_frames(own_1)
    grad_shape = shape_of(rows, frames, *block)
    grad_1 = call(
        second_forward,
        grad_shape,
        own_1,
        earlier_1,
        cotangent,
        low,
        kernels[1],
        norm_gains,
        scratch=patch_scratch(cells),
    )

    def with_neighbours(grad):
        later = earlier_frames(grad)
        above = from_above(jnp.concatenate([grad[rows - 2 :], later[rows - 2 :]], axis=1))
        return later, above

    share = channels // tiles
    part = shape_of(tiles // 2, TAPS, share, channels)
    later_1, above_1 = with_neighbours(grad_1)
    keep_1, send_1 = call(
        second_kernel_gradient, (part, part), own_1, earlier_1, grad_1, scratch=patch_scratch(cells)
    )
    came_1 = partner(send_1)
    grad_0 = call(
        second_backward,
        grad_shape,
        grad_1,
        later_1,
        above_1,
        kernels[1],
        norm_gains,
        pre_0,
        scratch=patch_scratch(cells),
    )
    keep_0, send_0 = call(
        first_kernel_gradient,
        (part, part),
        own_0,
        earlier_0,
        below_0,
        grad_0,
        scratch=patch_scratch(cells),
    )
    came_0 = partner(send_0)
    paired = call(
        add_pairs, shape_of(tiles // 2, 2 * TAPS, share, channels), keep_0, came_0, keep_1, came_1
    )
    by_core = [list(range(core, tiles, 2)) for core in range(2)]
    arrived = lax.all_to_all(
        paired, "tile", split_axis=0, concat_axis=0, tiled=True, axis_index_groups=by_core
    )
    later_0, above_0 = with_neighbours(grad_0)
    input_grad = call(
        first_backward,
        shape_of(frames, rows, *block),
        grad_0,
        later_0,
        above_0,
        kernels[0],
        scratch=patch_scratch(cells),
    )
    used = 2 * TAPS * share
    padded = -(-used // 128) * 128
    by_frame = call(
        sum_tiles,
        shape_of(groups, channels // groups, padded),
        arrived,
        scratch=(pltpu.VMEM((padded, channels), F32),),
    )
    spread = lax.all_to_all(by_frame, "frame", split_axis=0, concat_axis=0, tiled=True)
    scale = 1.0 / math.sqrt(cells * tiles * groups)
    summed = call(
        lambda *refs: sum_frames(scale, *refs),
        shape_of(used, channels // groups, dtype=F32),
        spread,
    )
    return (input_grad, summed.reshape(2 * TAPS, share, channels // groups))


def solution(mesh):
    in_specs = (
        P("frame", "tile", None, None),
        P("frame", "tile", None),
        P(),
        P(),
        P("frame", "tile", None, None),
    )
    out_specs = (P("frame", "tile", None, None), P(None, "tile", "frame"))
    return jax.shard_map(local, mesh=mesh, in_specs=in_specs, out_specs=out_specs, check_vma=False)
```

```python
import math

import jax
import jax.numpy as jnp
from jax import lax
from jax.experimental import pallas as pl
from jax.experimental.pallas import tpu as pltpu
from jax.sharding import PartitionSpec as P

EPS = 1e-06
TAPS = 27
F32 = jnp.float32
BF16 = jnp.bfloat16


def call(kernel, out_shape, *operands, scratch=()):
    return pl.pallas_call(
        kernel,
        out_shape=out_shape,
        scratch_shapes=list(scratch),
        compiler_params=pltpu.CompilerParams(vmem_limit_bytes=48 * 2**20),
    )(*operands)


def shifted_columns(block):
    shape = block.shape
    columns = shape[-2]
    flat = block.astype(F32).reshape(-1, shape[-1])
    column = lax.broadcasted_iota(jnp.int32, flat.shape, 0) % columns
    before = jnp.where(column == 0, 0.0, pltpu.roll(flat, 1, 0))
    after = jnp.where(column == columns - 1, 0.0, pltpu.roll(flat, flat.shape[0] - 1, 0))
    return before.astype(BF16).reshape(shape), block, after.astype(BF16).reshape(shape)


def fill(patches, window, frames, rows, sign, seams):
    columns, channels = window[0][0][0].shape
    for row in range(rows):
        for frame in range(frames):
            first = (row * frames + frame) * columns
            for tap in range(TAPS):
                depth, down, across = tap // 9, tap // 3 % 3, tap % 3
                if sign > 0:
                    source = window[row + down][frame + depth][across]
                else:
                    source = window[row + 2 - down][frame + 2 - depth][2 - across]
                    down = 2 - down
                seam = seams.get((row, down))
                if seam is not None:
                    source = jnp.where(seam, jnp.zeros_like(source), source)
                patches[first : first + columns, tap * channels : (tap + 1) * channels] = source


def window_of(rows):
    return [[shifted_columns(block) for block in row] for row in rows]


def block_rows(ref):
    return [[ref[row, frame] for frame in range(ref.shape[1])] for row in range(ref.shape[0])]


def silu_parts(pre_norm, gain):
    inverse = lax.rsqrt(jnp.mean(pre_norm * pre_norm, axis=-1, keepdims=True) + EPS)
    normed = pre_norm * inverse * gain
    return inverse, normed, 1.0 / (1.0 + jnp.exp(-normed))


def pre_norm_gradient(pre_norm, gain, upstream):
    inverse, normed, sigma = silu_parts(pre_norm, gain)
    scaled = gain * upstream * sigma * (1.0 + normed * (1.0 - sigma))
    mixed = jnp.mean(pre_norm * scaled, axis=-1, keepdims=True)
    return (inverse * scaled - pre_norm * inverse**3 * mixed).astype(BF16)


def at_last_tile():
    return lax.axis_index("tile") == lax.axis_size("tile") - 1


def first_rows(parts, below_ref, total):
    frames, rows = parts[0].shape[:2]
    skipped = (3 - len(parts)) * frames
    result = []
    for row in range(total):
        if row < rows:
            result.append([part[frame, row] for part in parts for frame in range(frames)])
        else:
            result.append(
                [
                    below_ref[(skipped + frame) * rows + row - rows]
                    for frame in range(len(parts) * frames)
                ]
            )
    return result


def forward(
    own_ref, earlier_ref, earliest_ref, below_ref, top_ref, first_kernel_ref, second_kernel_ref,
    gain_ref, next_ref, pre_ref, grad_ref, wide_patches, patches,
):
    frames, rows, columns, channels = own_ref.shape
    last = at_last_tile()
    window = window_of(first_rows((earliest_ref, earlier_ref, own_ref), below_ref, 2 * rows))
    wide, deep = 2 * rows - 2, 2 * frames
    fill(wide_patches, window, deep, wide, 1, {(rows - 2, 2): last, (rows - 1, 0): last})
    pre_norm = jnp.dot(
        wide_patches[...],
        first_kernel_ref[...].reshape(TAPS * channels, channels),
        preferred_element_type=F32,
    )
    _, normed, sigma = silu_parts(pre_norm, gain_ref[0:1])
    next_ref[...] = (normed * sigma).astype(BF16).reshape(next_ref.shape)
    own_cells = frames * columns
    for row in range(rows):
        start = row * deep * columns + own_cells
        pre_ref[row * own_cells : (row + 1) * own_cells] = pre_norm[start : start + own_cells]
    window = window_of(block_rows(next_ref))
    fill(patches, window, frames, rows, 1, {(rows - 3, 2): last, (rows - 2, 0): last})
    pre_norm = jnp.dot(
        patches[...],
        second_kernel_ref[...].reshape(TAPS * channels, channels),
        preferred_element_type=F32,
    )
    spread = []
    for row in range(rows):
        for frame in range(frames):
            if row < rows - 2:
                spread.append(top_ref[frame, row + 2])
            else:
                spread.append(below_ref[3 * frames * rows + frame * 2 + row - rows + 2])
    upstream = jnp.concatenate(spread, axis=0).astype(F32)
    grad_ref[...] = pre_norm_gradient(pre_norm, gain_ref[1:2], upstream).reshape(grad_ref.shape)


def backward_rows(own_ref, later_ref, above_ref, frames):
    rows = own_ref.shape[0]
    result = []
    for row in range(2):
        result.append([above_ref[row, frame] for frame in range(2 * frames)])
    for row in range(rows):
        result.append(
            [own_ref[row, frame] for frame in range(frames)]
            + [later_ref[row, frame] for frame in range(frames)]
        )
    return result


def back_product(patches, kernel_ref):
    turned = jnp.concatenate([kernel_ref[tap] for tap in range(TAPS)], axis=1)
    return lax.dot_general(
        patches[...], turned, (((1,), (1,)), ((), ())), preferred_element_type=F32
    )


def second_backward(
    own_ref, later_ref, above_ref, kernel_ref, gain_ref, pre_ref, grad_ref, patches
):
    rows, frames, columns, channels = own_ref.shape
    last = at_last_tile()
    window = window_of(backward_rows(own_ref, later_ref, above_ref, frames))
    fill(patches, window, frames, rows, -1, {(rows - 2, 2): last, (rows - 1, 0): last})
    upstream = back_product(patches, kernel_ref).astype(BF16).astype(F32)
    grad_ref[...] = pre_norm_gradient(pre_ref[...], gain_ref[0:1], upstream).reshape(grad_ref.shape)


def first_backward(own_ref, later_ref, above_ref, kernel_ref, out_ref, token_ref, patches):
    rows, frames, columns, channels = own_ref.shape
    first, last = lax.axis_index("tile") == 0, at_last_tile()
    window = window_of(backward_rows(own_ref, later_ref, above_ref, frames))
    fill(patches, window, frames, rows, -1, {(0, 0): first, (rows - 1, 2): last})
    grad = back_product(patches, kernel_ref).astype(BF16)
    for row in range(rows):
        for frame in range(frames):
            cell = (row * frames + frame) * columns
            out_ref[frame, row] = grad[cell : cell + columns]
    token_ref[...] = grad[: token_ref.shape[0]].astype(F32)


def split_gradient(patches, grad_ref, keep_ref, send_ref):
    chips, _, share, channels = keep_ref.shape
    odd = lax.axis_index("tile") % 2 == 1
    grad = grad_ref[...].reshape(-1, channels)
    for tap in range(TAPS):
        block = lax.dot_general(
            patches[:, tap * channels : (tap + 1) * channels],
            grad,
            (((0,), (0,)), ((), ())),
            preferred_element_type=F32,
        ).reshape(chips, 2, share, channels)
        even_part, odd_part = block[:, 0], block[:, 1]
        keep_ref[:, tap] = jnp.where(odd, odd_part, even_part).astype(BF16)
        send_ref[:, tap] = jnp.where(odd, even_part, odd_part).astype(BF16)


def second_kernel_gradient(next_ref, grad_ref, keep_ref, send_ref, patches):
    rows, frames, _, _ = grad_ref.shape
    last = at_last_tile()
    window = window_of(block_rows(next_ref))
    fill(patches, window, frames, rows, 1, {(rows - 3, 2): last, (rows - 2, 0): last})
    split_gradient(patches, grad_ref, keep_ref, send_ref)


def first_kernel_gradient(own_ref, earlier_ref, below_ref, grad_ref, keep_ref, send_ref, patches):
    frames, rows, columns, channels = own_ref.shape
    last = at_last_tile()
    window = window_of(first_rows((earlier_ref, own_ref), below_ref, rows + 2))
    fill(patches, window, frames, rows, 1, {(rows - 2, 2): last, (rows - 1, 0): last})
    split_gradient(patches, grad_ref, keep_ref, send_ref)


def add_pairs(keep_first, came_first, keep_second, came_second, out_ref):
    taps = keep_first.shape[1]
    out_ref[:, :taps] = (keep_first[...].astype(F32) + came_first[...].astype(F32)).astype(BF16)
    out_ref[:, taps:] = (keep_second[...].astype(F32) + came_second[...].astype(F32)).astype(BF16)


def sum_tiles(in_ref, token_ref, out_ref, rows_ref):
    del token_ref
    chips, taps, share, channels = in_ref.shape
    groups, width, _ = out_ref.shape
    total = in_ref[0].astype(F32)
    for chip in range(1, chips):
        total = total + in_ref[chip].astype(F32)
    rows_ref[...] = jnp.zeros_like(rows_ref)
    stride = rows_ref.shape[0] // share
    for row in range(share):
        rows_ref[row * stride : row * stride + taps] = total[:, row]
    out_ref[...] = rows_ref[...].T.reshape(groups, width, -1).astype(BF16)


def sum_frames(scale, in_ref, out_ref):
    groups = in_ref.shape[0]
    total = in_ref[0].astype(F32)
    for group in range(1, groups):
        total = total + in_ref[group].astype(F32)
    share, _, taps = out_ref.shape
    stride = total.shape[1] // share
    for row in range(share):
        out_ref[row] = total[:, row * stride : row * stride + taps] * scale


def shape_of(*dims, dtype=BF16):
    return jax.ShapeDtypeStruct(dims, dtype)


def local(saved_codes, saved_scales, kernels, norm_gains, cotangent):
    frames, rows, columns, channels = saved_codes.shape
    tiles, groups = lax.axis_size("tile"), lax.axis_size("frame")
    cells = frames * rows * columns
    block = (columns, channels)

    def patch_scratch(count):
        return (pltpu.VMEM((count, TAPS * channels), BF16),)

    def next_frames(value, steps):
        return lax.ppermute(value, "frame", [(i, i + steps) for i in range(groups - steps)])

    def earlier_frames(value):
        return lax.ppermute(value, "frame", [(i + 1, i) for i in range(groups - 1)])

    def from_below(value):
        return lax.ppermute(value, "tile", [((i + 1) % tiles, i) for i in range(tiles)])

    def from_above(value):
        return lax.ppermute(value, "tile", [(i, (i + 1) % tiles) for i in range(tiles)])

    def partner(value):
        return lax.ppermute(value, "tile", [(i, i ^ 1) for i in range(tiles)])

    own_0 = (saved_codes.astype(F32) * saved_scales[..., None]).astype(BF16)
    earlier_0, earliest_0 = next_frames(own_0, 1), next_frames(own_0, 2)
    sent = jnp.concatenate(
        [
            earliest_0.reshape(frames * rows, *block),
            earlier_0.reshape(frames * rows, *block),
            own_0.reshape(frames * rows, *block),
            cotangent[:, :2].reshape(frames * 2, *block),
        ],
        axis=0,
    )
    below = from_below(sent)
    wide = 2 * rows - 2
    grad_shape = shape_of(rows, frames, *block)
    next_1, pre_0, grad_1 = call(
        forward,
        (shape_of(wide, 2 * frames, *block), shape_of(cells, channels, dtype=F32), grad_shape),
        own_0,
        earlier_0,
        earliest_0,
        below,
        cotangent,
        kernels[0],
        kernels[1],
        norm_gains,
        scratch=patch_scratch(wide * 2 * frames * columns) + patch_scratch(cells),
    )

    def with_neighbours(grad):
        later = earlier_frames(grad)
        above = from_above(jnp.concatenate([grad[rows - 2 :], later[rows - 2 :]], axis=1))
        return later, above

    share = channels // tiles
    part = shape_of(tiles // 2, TAPS, share, channels)
    later_1, above_1 = with_neighbours(grad_1)
    keep_1, send_1 = call(
        second_kernel_gradient, (part, part), next_1, grad_1, scratch=patch_scratch(cells)
    )
    came_1 = partner(send_1)
    grad_0 = call(
        second_backward,
        grad_shape,
        grad_1,
        later_1,
        above_1,
        kernels[1],
        norm_gains,
        pre_0,
        scratch=patch_scratch(cells),
    )
    keep_0, send_0 = call(
        first_kernel_gradient,
        (part, part),
        own_0,
        earlier_0,
        below,
        grad_0,
        scratch=patch_scratch(cells),
    )
    came_0 = partner(send_0)
    paired = call(
        add_pairs, shape_of(tiles // 2, 2 * TAPS, share, channels), keep_0, came_0, keep_1, came_1
    )
    by_core = [list(range(core, tiles, 2)) for core in range(2)]
    arrived = lax.all_to_all(
        paired, "tile", split_axis=0, concat_axis=0, tiled=True, axis_index_groups=by_core
    )
    later_0, above_0 = with_neighbours(grad_0)
    input_grad, token = call(
        first_backward,
        (shape_of(frames, rows, *block), shape_of(8, channels, dtype=F32)),
        grad_0,
        later_0,
        above_0,
        kernels[0],
        scratch=patch_scratch(cells),
    )
    padded = -(-2 * TAPS // 32) * 32 * share
    by_frame = call(
        sum_tiles,
        shape_of(groups, channels // groups, padded),
        arrived,
        token,
        scratch=(pltpu.VMEM((padded, channels), F32),),
    )
    spread = lax.all_to_all(by_frame, "frame", split_axis=0, concat_axis=0, tiled=True)
    scale = 1.0 / math.sqrt(cells * tiles * groups)
    summed = call(
        lambda *refs: sum_frames(scale, *refs),
        shape_of(share, channels // groups, 2 * TAPS, dtype=F32),
        spread,
    )
    return (input_grad, jnp.transpose(summed, (2, 0, 1)))


def solution(mesh):
    in_specs = (
        P("frame", "tile", None, None),
        P("frame", "tile", None),
        P(),
        P(),
        P("frame", "tile", None, None),
    )
    out_specs = (P("frame", "tile", None, None), P(None, "tile", "frame"))
    return jax.shard_map(local, mesh=mesh, in_specs=in_specs, out_specs=out_specs, check_vma=False)
```

```python
import math

import jax
import jax.numpy as jnp
from jax import lax
from jax.experimental import pallas as pl
from jax.experimental.pallas import tpu as pltpu
from jax.sharding import PartitionSpec as P


EPS = 1e-06
TAPS = 27
F32 = jnp.float32
BF16 = jnp.bfloat16


def call(kernel, out_shape, *operands, scratch=()):
    return pl.pallas_call(
        kernel,
        out_shape=out_shape,
        scratch_shapes=list(scratch),
        compiler_params=pltpu.CompilerParams(vmem_limit_bytes=48 * 2**20),
    )(*operands)


def shifted_columns(block):
    shape = block.shape
    columns = shape[-2]
    flat = block.astype(F32).reshape(-1, shape[-1])
    column = lax.broadcasted_iota(jnp.int32, flat.shape, 0) % columns
    before = jnp.where(column == 0, 0.0, pltpu.roll(flat, 1, 0))
    after = jnp.where(column == columns - 1, 0.0, pltpu.roll(flat, flat.shape[0] - 1, 0))
    return before.astype(BF16).reshape(shape), block, after.astype(BF16).reshape(shape)


def fill(patches, window, frames, rows, sign, seams):
    columns, channels = window[0][0][0].shape
    for row in range(rows):
        for frame in range(frames):
            first = (row * frames + frame) * columns
            for tap in range(TAPS):
                depth, down, across = tap // 9, tap // 3 % 3, tap % 3
                if sign > 0:
                    source = window[row + down][frame + depth][across]
                else:
                    source = window[row + 2 - down][frame + 2 - depth][2 - across]
                    down = 2 - down
                seam = seams.get((row, down))
                if seam is not None:
                    source = jnp.where(seam, jnp.zeros_like(source), source)
                patches[first : first + columns, tap * channels : (tap + 1) * channels] = source


def window_of(rows):
    return [[shifted_columns(block) for block in row] for row in rows]


def block_rows(ref):
    return [[ref[row, frame] for frame in range(ref.shape[1])] for row in range(ref.shape[0])]


def product(patches, kernel_ref, chunk=256):
    weights = kernel_ref[...].reshape(-1, kernel_ref.shape[-1])
    pieces = [
        jnp.dot(patches[start : start + chunk], weights, preferred_element_type=F32)
        for start in range(0, patches.shape[0], chunk)
    ]
    return pieces


def silu_parts(pre_norm, gain):
    inverse = lax.rsqrt(jnp.mean(pre_norm * pre_norm, axis=-1, keepdims=True) + EPS)
    normed = pre_norm * inverse * gain
    return inverse, normed, 1.0 / (1.0 + jnp.exp(-normed))


def pre_norm_gradient(pre_norm, gain, upstream):
    inverse, normed, sigma = silu_parts(pre_norm, gain)
    scaled = gain * upstream * sigma * (1.0 + normed * (1.0 - sigma))
    mixed = jnp.mean(pre_norm * scaled, axis=-1, keepdims=True)
    return (inverse * scaled - pre_norm * inverse**3 * mixed).astype(BF16)


def at_last_tile():
    return lax.axis_index("tile") == lax.axis_size("tile") - 1


def first_rows(parts, below_ref, total):
    frames, rows = parts[0].shape[:2]
    skipped = (3 - len(parts)) * frames
    result = []
    for row in range(total):
        if row < rows:
            result.append([part[frame, row] for part in parts for frame in range(frames)])
        else:
            result.append(
                [
                    below_ref[(skipped + frame) * rows + row - rows]
                    for frame in range(len(parts) * frames)
                ]
            )
    return result


def forward(
    own_ref, earlier_ref, earliest_ref, below_ref, top_ref, first_kernel_ref, second_kernel_ref,
    gain_ref, next_ref, pre_ref, grad_ref, wide_patches, patches,
):
    frames, rows, columns, _ = own_ref.shape
    last = at_last_tile()
    window = window_of(first_rows((earliest_ref, earlier_ref, own_ref), below_ref, 2 * rows))
    wide, deep = 2 * rows - 2, 2 * frames
    fill(wide_patches, window, deep, wide, 1, {(rows - 2, 2): last, (rows - 1, 0): last})
    own_cells, blocks = frames * columns, 8
    for number, pre_norm in enumerate(product(wide_patches, first_kernel_ref, blocks * columns)):
        _, normed, sigma = silu_parts(pre_norm, gain_ref[0:1])
        value = (normed * sigma).astype(BF16)
        for block in range(blocks):
            row, frame = divmod(number * blocks + block, deep)
            cells = slice(block * columns, (block + 1) * columns)
            next_ref[row, frame] = value[cells]
            if row < rows and frame >= frames:
                start = row * own_cells + (frame - frames) * columns
                pre_ref[start : start + columns] = pre_norm[cells]
    window = window_of(block_rows(next_ref))
    fill(patches, window, frames, rows, 1, {(rows - 3, 2): last, (rows - 2, 0): last})
    (pre_norm,) = product(patches, second_kernel_ref)
    spread = []
    for row in range(rows):
        for frame in range(frames):
            if row < rows - 2:
                spread.append(top_ref[frame, row + 2])
            else:
                spread.append(below_ref[3 * frames * rows + frame * 2 + row - rows + 2])
    upstream = jnp.concatenate(spread, axis=0).astype(F32)
    grad_ref[...] = pre_norm_gradient(pre_norm, gain_ref[1:2], upstream).reshape(grad_ref.shape)


def backward_rows(own_ref, later_ref, above_ref, frames):
    rows = own_ref.shape[0]
    result = []
    for row in range(2):
        result.append([above_ref[row, frame] for frame in range(2 * frames)])
    for row in range(rows):
        result.append(
            [own_ref[row, frame] for frame in range(frames)]
            + [later_ref[row, frame] for frame in range(frames)]
        )
    return result


def back_product(patches, kernel_ref):
    turned = jnp.concatenate([kernel_ref[tap] for tap in range(TAPS)], axis=1)
    return lax.dot_general(
        patches[...], turned, (((1,), (1,)), ((), ())), preferred_element_type=F32
    )


def second_backward(
    own_ref, later_ref, above_ref, kernel_ref, gain_ref, pre_ref, token_ref, grad_ref, patches
):
    del token_ref
    rows, frames, _, _ = own_ref.shape
    last = at_last_tile()
    window = window_of(backward_rows(own_ref, later_ref, above_ref, frames))
    fill(patches, window, frames, rows, -1, {(rows - 2, 2): last, (rows - 1, 0): last})
    upstream = back_product(patches, kernel_ref).astype(BF16).astype(F32)
    grad_ref[...] = pre_norm_gradient(pre_ref[...], gain_ref[0:1], upstream).reshape(grad_ref.shape)


def first_backward(own_ref, later_ref, above_ref, kernel_ref, out_ref, token_ref, patches):
    rows, frames, columns, _ = own_ref.shape
    first, last = lax.axis_index("tile") == 0, at_last_tile()
    window = window_of(backward_rows(own_ref, later_ref, above_ref, frames))
    fill(patches, window, frames, rows, -1, {(0, 0): first, (rows - 1, 2): last})
    grad = back_product(patches, kernel_ref).astype(BF16)
    for row in range(rows):
        for frame in range(frames):
            cell = (row * frames + frame) * columns
            out_ref[frame, row] = grad[cell : cell + columns]
    token_ref[...] = grad[: token_ref.shape[0]].astype(F32)


def split_gradient(patches, grad_ref, keep_ref, send_ref):
    chips, _, share, channels = keep_ref.shape
    odd = lax.axis_index("tile") % 2 == 1
    grad = grad_ref[...].reshape(-1, channels)
    for tap in range(TAPS):
        block = lax.dot_general(
            patches[:, tap * channels : (tap + 1) * channels],
            grad,
            (((0,), (0,)), ((), ())),
            preferred_element_type=F32,
        ).reshape(chips, 2, share, channels)
        even_part, odd_part = block[:, 0], block[:, 1]
        keep_ref[:, tap] = jnp.where(odd, odd_part, even_part).astype(BF16)
        send_ref[:, tap] = jnp.where(odd, even_part, odd_part).astype(BF16)


def second_kernel_gradient(next_ref, grad_ref, keep_ref, send_ref, token_ref, patches):
    rows, frames, _, _ = grad_ref.shape
    last = at_last_tile()
    window = window_of(block_rows(next_ref))
    fill(patches, window, frames, rows, 1, {(rows - 3, 2): last, (rows - 2, 0): last})
    split_gradient(patches, grad_ref, keep_ref, send_ref)
    token_ref[...] = jnp.zeros_like(token_ref)


def first_kernel_gradient(own_ref, earlier_ref, below_ref, grad_ref, keep_ref, send_ref, patches):
    frames, rows, _, _ = own_ref.shape
    last = at_last_tile()
    window = window_of(first_rows((earlier_ref, own_ref), below_ref, rows + 2))
    fill(patches, window, frames, rows, 1, {(rows - 2, 2): last, (rows - 1, 0): last})
    split_gradient(patches, grad_ref, keep_ref, send_ref)


def pack_rows(own_ref, later_ref, token_ref, out_ref):
    del token_ref
    frames, first = own_ref.shape[1], own_ref.shape[0] - out_ref.shape[0]
    out_ref[:, :frames] = own_ref[first:]
    out_ref[:, frames:] = later_ref[first:]


def add_pair(keep_ref, came_ref, out_ref, token_ref):
    out_ref[...] = (keep_ref[...].astype(F32) + came_ref[...].astype(F32)).astype(BF16)
    token_ref[...] = jnp.zeros_like(token_ref)


def sum_tiles(first_ref, second_ref, token_ref, out_ref, rows_ref):
    del token_ref
    chips, taps, share, _ = first_ref.shape
    groups, width, _ = out_ref.shape
    rows_ref[...] = jnp.zeros_like(rows_ref)
    stride = rows_ref.shape[0] // share
    for layer, in_ref in enumerate((first_ref, second_ref)):
        total = in_ref[0].astype(F32)
        for chip in range(1, chips):
            total = total + in_ref[chip].astype(F32)
        for row in range(share):
            start = row * stride + layer * taps
            rows_ref[start : start + taps] = total[:, row]
    out_ref[...] = rows_ref[...].T.reshape(groups, width, -1).astype(BF16)


def sum_frames(scale, in_ref, out_ref):
    groups = in_ref.shape[0]
    total = in_ref[0].astype(F32)
    for group in range(1, groups):
        total = total + in_ref[group].astype(F32)
    share, _, taps = out_ref.shape
    stride = total.shape[1] // share
    for row in range(share):
        out_ref[row] = total[:, row * stride : row * stride + taps] * scale


def shape_of(*dims, dtype=BF16):
    return jax.ShapeDtypeStruct(dims, dtype)


def local(saved_codes, saved_scales, kernels, norm_gains, cotangent):
    frames, rows, columns, channels = saved_codes.shape
    tiles, groups = lax.axis_size("tile"), lax.axis_size("frame")
    cells = frames * rows * columns
    block = (columns, channels)

    def patch_scratch(count):
        return (pltpu.VMEM((count, TAPS * channels), BF16),)

    def next_frames(value, steps):
        return lax.ppermute(value, "frame", [(i, i + steps) for i in range(groups - steps)])

    def earlier_frames(value):
        return lax.ppermute(value, "frame", [(i + 1, i) for i in range(groups - 1)])

    def from_below(value):
        return lax.ppermute(value, "tile", [((i + 1) % tiles, i) for i in range(tiles)])

    def from_above(value):
        return lax.ppermute(value, "tile", [(i, (i + 1) % tiles) for i in range(tiles)])

    def partner(value):
        return lax.ppermute(value, "tile", [(i, i ^ 1) for i in range(tiles)])

    own_0 = (saved_codes.astype(F32) * saved_scales[..., None]).astype(BF16)
    earlier_0, earliest_0 = next_frames(own_0, 1), next_frames(own_0, 2)
    sent = jnp.concatenate(
        [
            earliest_0.reshape(frames * rows, *block),
            earlier_0.reshape(frames * rows, *block),
            own_0.reshape(frames * rows, *block),
            cotangent[:, :2].reshape(frames * 2, *block),
        ],
        axis=0,
    )
    below = from_below(sent)
    wide = 2 * rows - 2
    grad_shape = shape_of(rows, frames, *block)
    next_1, pre_0, grad_1 = call(
        forward,
        (shape_of(wide, 2 * frames, *block), shape_of(cells, channels, dtype=F32), grad_shape),
        own_0,
        earlier_0,
        earliest_0,
        below,
        cotangent,
        kernels[0],
        kernels[1],
        norm_gains,
        scratch=patch_scratch(wide * 2 * frames * columns) + patch_scratch(cells),
    )

    share = channels // tiles
    part = shape_of(tiles // 2, TAPS, share, channels)
    mark = shape_of(8, channels, dtype=F32)

    def with_neighbours(later, grad, token):
        edge = shape_of(2, 2 * frames, *block)
        packed = call(pack_rows, edge, grad, later, token)
        return from_above(packed)

    by_core = [list(range(core, tiles, 2)) for core in range(2)]

    def sent_and_paired(keep, send):
        came = partner(send)
        paired, token = call(add_pair, (part, mark), keep, came)
        arrived = lax.all_to_all(
            paired, "tile", split_axis=0, concat_axis=0, tiled=True, axis_index_groups=by_core
        )
        return arrived, token

    later_1 = earlier_frames(grad_1)
    keep_1, send_1, token = call(
        second_kernel_gradient, (part, part, mark), next_1, grad_1, scratch=patch_scratch(cells)
    )
    above_1 = with_neighbours(later_1, grad_1, token)
    arrived_1, token = sent_and_paired(keep_1, send_1)
    grad_0 = call(
        second_backward,
        grad_shape,
        grad_1,
        later_1,
        above_1,
        kernels[1],
        norm_gains,
        pre_0,
        token,
        scratch=patch_scratch(cells),
    )
    keep_0, send_0 = call(
        first_kernel_gradient,
        (part, part),
        own_0,
        earlier_0,
        below,
        grad_0,
        scratch=patch_scratch(cells),
    )
    arrived_0, token = sent_and_paired(keep_0, send_0)
    later_0 = earlier_frames(grad_0)
    above_0 = with_neighbours(later_0, grad_0, token)
    input_grad, token = call(
        first_backward,
        (shape_of(frames, rows, *block), mark),
        grad_0,
        later_0,
        above_0,
        kernels[0],
        scratch=patch_scratch(cells),
    )
    padded = -(-2 * TAPS // 32) * 32 * share
    by_frame = call(
        sum_tiles,
        shape_of(groups, channels // groups, padded),
        arrived_0,
        arrived_1,
        token,
        scratch=(pltpu.VMEM((padded, channels), F32),),
    )
    spread = lax.all_to_all(by_frame, "frame", split_axis=0, concat_axis=0, tiled=True)
    scale = 1.0 / math.sqrt(cells * tiles * groups)
    summed = call(
        lambda *refs: sum_frames(scale, *refs),
        shape_of(share, channels // groups, 2 * TAPS, dtype=F32),
        spread,
    )
    return (input_grad, jnp.transpose(summed, (2, 0, 1)))


def solution(mesh):
    in_specs = (
        P("frame", "tile", None, None),
        P("frame", "tile", None),
        P(),
        P(),
        P("frame", "tile", None, None),
    )
    out_specs = (P("frame", "tile", None, None), P(None, "tile", "frame"))

    return jax.shard_map(local, mesh=mesh, in_specs=in_specs, out_specs=out_specs, check_vma=False)
```

```python
import math

import jax
import jax.numpy as jnp
from jax import lax
from jax.experimental import pallas as pl
from jax.experimental.pallas import tpu as pltpu
from jax.sharding import PartitionSpec as P


EPS = 1e-06
TAPS = 27
F32 = jnp.float32
BF16 = jnp.bfloat16


def call(kernel, out_shape, *operands, scratch=()):
    return pl.pallas_call(
        kernel,
        out_shape=out_shape,
        scratch_shapes=list(scratch),
        compiler_params=pltpu.CompilerParams(vmem_limit_bytes=48 * 2**20),
    )(*operands)


def shifted_columns(block):
    shape = block.shape
    columns = shape[-2]
    flat = block.astype(F32).reshape(-1, shape[-1])
    column = lax.broadcasted_iota(jnp.int32, flat.shape, 0) % columns
    before = jnp.where(column == 0, 0.0, pltpu.roll(flat, 1, 0))
    after = jnp.where(column == columns - 1, 0.0, pltpu.roll(flat, flat.shape[0] - 1, 0))
    return before.astype(BF16).reshape(shape), block, after.astype(BF16).reshape(shape)


def store_columns(store, window, order, seams):
    for row, blocks in enumerate(window):
        for frame, triple in enumerate(blocks):
            store[row, frame] = jnp.concatenate([triple[across] for across in order], axis=1)
    for extra, ((row, offset), seam) in enumerate(seams.items()):
        for frame in range(store.shape[1]):
            source = store[row + offset, frame]
            store[len(window) + extra, frame] = jnp.where(seam, jnp.zeros_like(source), source)


def side_by_side(store, seams, rows, frames, sign, index):
    depth, down = divmod(index, 3)
    if sign < 0:
        depth, down = 2 - depth, 2 - down
    extra, total = list(seams), store.shape[0] - len(seams)
    pieces = []
    for row in rows:
        place = total + extra.index((row, down)) if (row, down) in seams else row + down
        pieces.append(store[place, depth : depth + frames].reshape(-1, store.shape[-1]))
    return jnp.concatenate(pieces, axis=0)


def product(store, seams, rows, frames, sign, kernel_ref):
    total = None
    for index in range(0, 9, 2):
        members = range(index, min(index + 2, 9))
        cells = jnp.concatenate(
            [side_by_side(store, seams, rows, frames, sign, member) for member in members], axis=1
        )
        taps = range(3 * members[0], 3 * members[-1] + 3)
        if sign > 0:
            weights = kernel_ref[taps[0] : taps[-1] + 1].reshape(-1, kernel_ref.shape[-1])
            part = jnp.dot(cells, weights, preferred_element_type=F32)
        else:
            weights = jnp.concatenate([kernel_ref[tap] for tap in taps], axis=1)
            part = lax.dot_general(
                cells, weights, (((1,), (1,)), ((), ())), preferred_element_type=F32
            )
        total = part if total is None else total + part
    return total


def window_of(rows):
    return [[shifted_columns(block) for block in row] for row in rows]


def block_rows(ref):
    return [[ref[row, frame] for frame in range(ref.shape[1])] for row in range(ref.shape[0])]


def silu_parts(pre_norm, gain):
    inverse = lax.rsqrt(jnp.mean(pre_norm * pre_norm, axis=-1, keepdims=True) + EPS)
    normed = pre_norm * inverse * gain
    return inverse, normed, 1.0 / (1.0 + jnp.exp(-normed))


def pre_norm_gradient(pre_norm, gain, upstream):
    inverse, normed, sigma = silu_parts(pre_norm, gain)
    scaled = gain * upstream * sigma * (1.0 + normed * (1.0 - sigma))
    mixed = jnp.mean(pre_norm * scaled, axis=-1, keepdims=True)
    return (inverse * scaled - pre_norm * inverse**3 * mixed).astype(BF16)


def at_last_tile():
    return lax.axis_index("tile") == lax.axis_size("tile") - 1


def first_rows(parts, below_ref, total):
    frames, rows = parts[0].shape[:2]
    skipped = (3 - len(parts)) * frames
    result = []
    for row in range(total):
        if row < rows:
            result.append([part[frame, row] for part in parts for frame in range(frames)])
        else:
            result.append(
                [
                    below_ref[(skipped + frame) * rows + row - rows]
                    for frame in range(len(parts) * frames)
                ]
            )
    return result


def forward(
    own_ref, earlier_ref, earliest_ref, below_ref, top_ref, first_kernel_ref, second_kernel_ref,
    gain_ref, next_ref, pre_ref, grad_ref, wide_store, store,
):
    frames, rows, columns, _ = own_ref.shape
    last = at_last_tile()
    window = window_of(first_rows((earliest_ref, earlier_ref, own_ref), below_ref, 2 * rows))
    wide, deep = 2 * rows - 2, 2 * frames
    seams = {(rows - 2, 2): last, (rows - 1, 0): last}
    store_columns(wide_store, window, (0, 1, 2), seams)
    own_cells = frames * columns
    for first in range(0, wide, 2):
        pre_norm = product(wide_store, seams, (first, first + 1), deep, 1, first_kernel_ref)
        _, normed, sigma = silu_parts(pre_norm, gain_ref[0:1])
        value = (normed * sigma).astype(BF16)
        for block in range(2 * deep):
            row, frame = first + block // deep, block % deep
            cells = slice(block * columns, (block + 1) * columns)
            next_ref[row, frame] = value[cells]
            if row < rows and frame >= frames:
                start = row * own_cells + (frame - frames) * columns
                pre_ref[start : start + columns] = pre_norm[cells]
    seams = {(rows - 3, 2): last, (rows - 2, 0): last}
    store_columns(store, window_of(block_rows(next_ref)), (0, 1, 2), seams)
    pre_norm = product(store, seams, range(rows), frames, 1, second_kernel_ref)
    spread = []
    for row in range(rows):
        for frame in range(frames):
            if row < rows - 2:
                spread.append(top_ref[frame, row + 2])
            else:
                spread.append(below_ref[3 * frames * rows + frame * 2 + row - rows + 2])
    upstream = jnp.concatenate(spread, axis=0).astype(F32)
    grad_ref[...] = pre_norm_gradient(pre_norm, gain_ref[1:2], upstream).reshape(grad_ref.shape)


def backward_rows(own_ref, later_ref, above_ref, frames):
    rows = own_ref.shape[0]
    result = []
    for row in range(2):
        result.append([above_ref[row, frame] for frame in range(2 * frames)])
    for row in range(rows):
        result.append(
            [own_ref[row, frame] for frame in range(frames)]
            + [later_ref[row, frame] for frame in range(frames)]
        )
    return result


def second_backward(
    own_ref, later_ref, above_ref, kernel_ref, gain_ref, pre_ref, token_ref, grad_ref, store
):
    del token_ref
    rows, frames, _, _ = own_ref.shape
    last = at_last_tile()
    seams = {(rows - 2, 2): last, (rows - 1, 0): last}
    window = window_of(backward_rows(own_ref, later_ref, above_ref, frames))
    store_columns(store, window, (2, 1, 0), seams)
    upstream = product(store, seams, range(rows), frames, -1, kernel_ref).astype(BF16).astype(F32)
    grad_ref[...] = pre_norm_gradient(pre_ref[...], gain_ref[0:1], upstream).reshape(grad_ref.shape)


def first_backward(own_ref, later_ref, above_ref, kernel_ref, out_ref, token_ref, store):
    rows, frames, columns, _ = own_ref.shape
    seams = {(0, 0): lax.axis_index("tile") == 0, (rows - 1, 2): at_last_tile()}
    window = window_of(backward_rows(own_ref, later_ref, above_ref, frames))
    store_columns(store, window, (2, 1, 0), seams)
    grad = product(store, seams, range(rows), frames, -1, kernel_ref).astype(BF16)
    for row in range(rows):
        for frame in range(frames):
            cell = (row * frames + frame) * columns
            out_ref[frame, row] = grad[cell : cell + columns]
    token_ref[...] = grad[: token_ref.shape[0]].astype(F32)


def split_gradient(store, seams, grad_ref, keep_ref, send_ref):
    chips, _, share, channels = keep_ref.shape
    rows, frames, _, _ = grad_ref.shape
    odd = lax.axis_index("tile") % 2 == 1
    grad = grad_ref[...].reshape(-1, channels)
    for index in range(9):
        blocks = lax.dot_general(
            side_by_side(store, seams, range(rows), frames, 1, index),
            grad,
            (((0,), (0,)), ((), ())),
            preferred_element_type=F32,
        )
        for across in range(3):
            block = blocks[across * channels : (across + 1) * channels]
            block = block.reshape(chips, 2, share, channels)
            even_part, odd_part = block[:, 0], block[:, 1]
            tap = 3 * index + across
            keep_ref[:, tap] = jnp.where(odd, odd_part, even_part).astype(BF16)
            send_ref[:, tap] = jnp.where(odd, even_part, odd_part).astype(BF16)


def second_kernel_gradient(next_ref, grad_ref, keep_ref, send_ref, token_ref, store):
    rows = grad_ref.shape[0]
    last = at_last_tile()
    seams = {(rows - 3, 2): last, (rows - 2, 0): last}
    store_columns(store, window_of(block_rows(next_ref)), (0, 1, 2), seams)
    split_gradient(store, seams, grad_ref, keep_ref, send_ref)
    token_ref[...] = jnp.zeros_like(token_ref)


def first_kernel_gradient(own_ref, earlier_ref, below_ref, grad_ref, keep_ref, send_ref, store):
    rows = grad_ref.shape[0]
    last = at_last_tile()
    seams = {(rows - 2, 2): last, (rows - 1, 0): last}
    window = window_of(first_rows((earlier_ref, own_ref), below_ref, rows + 2))
    store_columns(store, window, (0, 1, 2), seams)
    split_gradient(store, seams, grad_ref, keep_ref, send_ref)


def pack_rows(own_ref, later_ref, token_ref, out_ref):
    del token_ref
    frames, first = own_ref.shape[1], own_ref.shape[0] - out_ref.shape[0]
    out_ref[:, :frames] = own_ref[first:]
    out_ref[:, frames:] = later_ref[first:]


def add_pair(keep_ref, came_ref, out_ref, token_ref):
    out_ref[...] = (keep_ref[...].astype(F32) + came_ref[...].astype(F32)).astype(BF16)
    token_ref[...] = jnp.zeros_like(token_ref)


def sum_tiles(first_ref, second_ref, token_ref, out_ref, rows_ref):
    del token_ref
    chips, taps, share, _ = first_ref.shape
    groups, width, _ = out_ref.shape
    rows_ref[...] = jnp.zeros_like(rows_ref)
    stride = rows_ref.shape[0] // share
    for layer, in_ref in enumerate((first_ref, second_ref)):
        total = in_ref[0].astype(F32)
        for chip in range(1, chips):
            total = total + in_ref[chip].astype(F32)
        for row in range(share):
            start = row * stride + layer * taps
            rows_ref[start : start + taps] = total[:, row]
    out_ref[...] = rows_ref[...].T.reshape(groups, width, -1).astype(BF16)


def sum_frames(scale, in_ref, out_ref):
    groups = in_ref.shape[0]
    total = in_ref[0].astype(F32)
    for group in range(1, groups):
        total = total + in_ref[group].astype(F32)
    share, _, taps = out_ref.shape
    stride = total.shape[1] // share
    for row in range(share):
        out_ref[row] = total[:, row * stride : row * stride + taps] * scale


def shape_of(*dims, dtype=BF16):
    return jax.ShapeDtypeStruct(dims, dtype)


def local(saved_codes, saved_scales, kernels, norm_gains, cotangent):
    frames, rows, columns, channels = saved_codes.shape
    tiles, groups = lax.axis_size("tile"), lax.axis_size("frame")
    cells = frames * rows * columns
    block = (columns, channels)

    def column_store(window_rows, window_frames):
        return (pltpu.VMEM((window_rows + 2, window_frames, columns, 3 * channels), BF16),)

    def next_frames(value, steps):
        return lax.ppermute(value, "frame", [(i, i + steps) for i in range(groups - steps)])

    def earlier_frames(value):
        return lax.ppermute(value, "frame", [(i + 1, i) for i in range(groups - 1)])

    def from_below(value):
        return lax.ppermute(value, "tile", [((i + 1) % tiles, i) for i in range(tiles)])

    def from_above(value):
        return lax.ppermute(value, "tile", [(i, (i + 1) % tiles) for i in range(tiles)])

    def partner(value):
        return lax.ppermute(value, "tile", [(i, i ^ 1) for i in range(tiles)])

    own_0 = (saved_codes.astype(F32) * saved_scales[..., None]).astype(BF16)
    earlier_0, earliest_0 = next_frames(own_0, 1), next_frames(own_0, 2)
    sent = jnp.concatenate(
        [
            earliest_0.reshape(frames * rows, *block),
            earlier_0.reshape(frames * rows, *block),
            own_0.reshape(frames * rows, *block),
            cotangent[:, :2].reshape(frames * 2, *block),
        ],
        axis=0,
    )
    below = from_below(sent)
    wide = 2 * rows - 2
    grad_shape = shape_of(rows, frames, *block)
    next_1, pre_0, grad_1 = call(
        forward,
        (shape_of(wide, 2 * frames, *block), shape_of(cells, channels, dtype=F32), grad_shape),
        own_0,
        earlier_0,
        earliest_0,
        below,
        cotangent,
        kernels[0],
        kernels[1],
        norm_gains,
        scratch=column_store(2 * rows, 3 * frames) + column_store(wide, 2 * frames),
    )

    share = channels // tiles
    part = shape_of(tiles // 2, TAPS, share, channels)
    mark = shape_of(8, channels, dtype=F32)

    def with_neighbours(later, grad, token):
        edge = shape_of(2, 2 * frames, *block)
        packed = call(pack_rows, edge, grad, later, token)
        return from_above(packed)

    by_core = [list(range(core, tiles, 2)) for core in range(2)]

    def sent_and_paired(keep, send):
        came = partner(send)
        paired, token = call(add_pair, (part, mark), keep, came)
        arrived = lax.all_to_all(
            paired, "tile", split_axis=0, concat_axis=0, tiled=True, axis_index_groups=by_core
        )
        return arrived, token

    later_1 = earlier_frames(grad_1)
    keep_1, send_1, token = call(
        second_kernel_gradient, (part, part, mark), next_1, grad_1, scratch=column_store(rows + 2, 2 * frames)
    )
    above_1 = with_neighbours(later_1, grad_1, token)
    arrived_1, token = sent_and_paired(keep_1, send_1)
    grad_0 = call(
        second_backward,
        grad_shape,
        grad_1,
        later_1,
        above_1,
        kernels[1],
        norm_gains,
        pre_0,
        token,
        scratch=column_store(rows + 2, 2 * frames),
    )
    keep_0, send_0 = call(
        first_kernel_gradient,
        (part, part),
        own_0,
        earlier_0,
        below,
        grad_0,
        scratch=column_store(rows + 2, 2 * frames),
    )
    arrived_0, token = sent_and_paired(keep_0, send_0)
    later_0 = earlier_frames(grad_0)
    above_0 = with_neighbours(later_0, grad_0, token)
    input_grad, token = call(
        first_backward,
        (shape_of(frames, rows, *block), mark),
        grad_0,
        later_0,
        above_0,
        kernels[0],
        scratch=column_store(rows + 2, 2 * frames),
    )
    padded = -(-2 * TAPS // 32) * 32 * share
    by_frame = call(
        sum_tiles,
        shape_of(groups, channels // groups, padded),
        arrived_0,
        arrived_1,
        token,
        scratch=(pltpu.VMEM((padded, channels), F32),),
    )
    spread = lax.all_to_all(by_frame, "frame", split_axis=0, concat_axis=0, tiled=True)
    scale = 1.0 / math.sqrt(cells * tiles * groups)
    summed = call(
        lambda *refs: sum_frames(scale, *refs),
        shape_of(share, channels // groups, 2 * TAPS, dtype=F32),
        spread,
    )
    return (input_grad, jnp.transpose(summed, (2, 0, 1)))


def solution(mesh):
    in_specs = (
        P("frame", "tile", None, None),
        P("frame", "tile", None),
        P(),
        P(),
        P("frame", "tile", None, None),
    )
    out_specs = (P("frame", "tile", None, None), P(None, "tile", "frame"))

    return jax.shard_map(local, mesh=mesh, in_specs=in_specs, out_specs=out_specs, check_vma=False)
```

```python
import math

import jax
import jax.numpy as jnp
from jax import lax
from jax.experimental import pallas as pl
from jax.experimental.pallas import tpu as pltpu
from jax.sharding import PartitionSpec as P


EPS = 1e-06
TAPS = 27
SLOTS = 28
F32 = jnp.float32
BF16 = jnp.bfloat16


def call(kernel, out_shape, *operands, scratch=()):
    return pl.pallas_call(
        kernel,
        out_shape=out_shape,
        scratch_shapes=list(scratch),
        compiler_params=pltpu.CompilerParams(vmem_limit_bytes=48 * 2**20),
    )(*operands)


def shifted_columns(block):
    shape = block.shape
    columns = shape[-2]
    flat = block.astype(F32).reshape(-1, shape[-1])
    column = lax.broadcasted_iota(jnp.int32, flat.shape, 0) % columns
    before = jnp.where(column == 0, 0.0, pltpu.roll(flat, 1, 0))
    after = jnp.where(column == columns - 1, 0.0, pltpu.roll(flat, flat.shape[0] - 1, 0))
    return before.astype(BF16).reshape(shape), block, after.astype(BF16).reshape(shape)


def store_columns(store, window, order, seams):
    for row, blocks in enumerate(window):
        for frame, triple in enumerate(blocks):
            store[row, frame] = jnp.concatenate([triple[across] for across in order], axis=1)
    for extra, ((row, offset), seam) in enumerate(seams.items()):
        for frame in range(store.shape[1]):
            source = store[row + offset, frame]
            store[len(window) + extra, frame] = jnp.where(seam, jnp.zeros_like(source), source)


def side_by_side(store, seams, rows, frames, sign, index):
    depth, down = divmod(index, 3)
    if sign < 0:
        depth, down = 2 - depth, 2 - down
    extra, total = list(seams), store.shape[0] - len(seams)
    pieces = []
    for row in rows:
        place = total + extra.index((row, down)) if (row, down) in seams else row + down
        pieces.append(store[place, depth : depth + frames].reshape(-1, store.shape[-1]))
    return jnp.concatenate(pieces, axis=0)


def product(store, seams, rows, frames, sign, kernel_ref):
    total = None
    for index in range(0, 9, 2):
        members = range(index, min(index + 2, 9))
        cells = jnp.concatenate(
            [side_by_side(store, seams, rows, frames, sign, member) for member in members], axis=1
        )
        taps = range(3 * members[0], 3 * members[-1] + 3)
        if sign > 0:
            weights = kernel_ref[taps[0] : taps[-1] + 1].reshape(-1, kernel_ref.shape[-1])
            part = jnp.dot(cells, weights, preferred_element_type=F32)
        else:
            weights = jnp.concatenate([kernel_ref[tap] for tap in taps], axis=1)
            part = lax.dot_general(
                cells, weights, (((1,), (1,)), ((), ())), preferred_element_type=F32
            )
        total = part if total is None else total + part
    return total


def window_of(rows):
    return [[shifted_columns(block) for block in row] for row in rows]


def block_rows(ref):
    return [[ref[row, frame] for frame in range(ref.shape[1])] for row in range(ref.shape[0])]


def silu_parts(pre_norm, gain):
    inverse = lax.rsqrt(jnp.mean(pre_norm * pre_norm, axis=-1, keepdims=True) + EPS)
    normed = pre_norm * inverse * gain
    return inverse, normed, 1.0 / (1.0 + jnp.exp(-normed))


def pre_norm_gradient(pre_norm, gain, upstream):
    inverse, normed, sigma = silu_parts(pre_norm, gain)
    scaled = gain * upstream * sigma * (1.0 + normed * (1.0 - sigma))
    mixed = jnp.mean(pre_norm * scaled, axis=-1, keepdims=True)
    return (inverse * scaled - pre_norm * inverse**3 * mixed).astype(BF16)


def at_last_tile():
    return lax.axis_index("tile") == lax.axis_size("tile") - 1


def first_rows(parts, below_ref, total):
    frames, rows = parts[0].shape[:2]
    skipped = (3 - len(parts)) * frames
    result = []
    for row in range(total):
        if row < rows:
            result.append([part[frame, row] for part in parts for frame in range(frames)])
        else:
            result.append(
                [
                    below_ref[(skipped + frame) * rows + row - rows]
                    for frame in range(len(parts) * frames)
                ]
            )
    return result


def forward(
    own_ref, earlier_ref, earliest_ref, below_ref, top_ref, first_kernel_ref, second_kernel_ref,
    gain_ref, next_ref, pre_ref, grad_ref, wide_store, store,
):
    frames, rows, columns, _ = own_ref.shape
    last = at_last_tile()
    window = window_of(first_rows((earliest_ref, earlier_ref, own_ref), below_ref, 2 * rows))
    wide, deep = 2 * rows - 2, 2 * frames
    seams = {(rows - 2, 2): last, (rows - 1, 0): last}
    store_columns(wide_store, window, (0, 1, 2), seams)
    own_cells = frames * columns
    for first in range(0, wide, 2):
        pre_norm = product(wide_store, seams, (first, first + 1), deep, 1, first_kernel_ref)
        _, normed, sigma = silu_parts(pre_norm, gain_ref[0:1])
        value = (normed * sigma).astype(BF16)
        for block in range(2 * deep):
            row, frame = first + block // deep, block % deep
            cells = slice(block * columns, (block + 1) * columns)
            next_ref[row, frame] = value[cells]
            if row < rows and frame >= frames:
                start = row * own_cells + (frame - frames) * columns
                pre_ref[start : start + columns] = pre_norm[cells]
    seams = {(rows - 3, 2): last, (rows - 2, 0): last}
    store_columns(store, window_of(block_rows(next_ref)), (0, 1, 2), seams)
    pre_norm = product(store, seams, range(rows), frames, 1, second_kernel_ref)
    spread = []
    for row in range(rows):
        for frame in range(frames):
            if row < rows - 2:
                spread.append(top_ref[frame, row + 2])
            else:
                spread.append(below_ref[3 * frames * rows + frame * 2 + row - rows + 2])
    upstream = jnp.concatenate(spread, axis=0).astype(F32)
    grad_ref[...] = pre_norm_gradient(pre_norm, gain_ref[1:2], upstream).reshape(grad_ref.shape)


def backward_rows(own_ref, later_ref, above_ref, frames):
    rows = own_ref.shape[0]
    result = []
    for row in range(2):
        result.append([above_ref[row, frame] for frame in range(2 * frames)])
    for row in range(rows):
        result.append(
            [own_ref[row, frame] for frame in range(frames)]
            + [later_ref[row, frame] for frame in range(frames)]
        )
    return result


def second_backward(
    own_ref, later_ref, above_ref, kernel_ref, gain_ref, pre_ref, grad_ref, store
):
    rows, frames, _, _ = own_ref.shape
    last = at_last_tile()
    seams = {(rows - 2, 2): last, (rows - 1, 0): last}
    window = window_of(backward_rows(own_ref, later_ref, above_ref, frames))
    store_columns(store, window, (2, 1, 0), seams)
    upstream = product(store, seams, range(rows), frames, -1, kernel_ref).astype(BF16).astype(F32)
    grad_ref[...] = pre_norm_gradient(pre_ref[...], gain_ref[0:1], upstream).reshape(grad_ref.shape)


def first_backward(own_ref, later_ref, above_ref, kernel_ref, out_ref, token_ref, store):
    rows, frames, columns, _ = own_ref.shape
    seams = {(0, 0): lax.axis_index("tile") == 0, (rows - 1, 2): at_last_tile()}
    window = window_of(backward_rows(own_ref, later_ref, above_ref, frames))
    store_columns(store, window, (2, 1, 0), seams)
    grad = product(store, seams, range(rows), frames, -1, kernel_ref).astype(BF16)
    for row in range(rows):
        for frame in range(frames):
            cell = (row * frames + frame) * columns
            out_ref[frame, row] = grad[cell : cell + columns]
    token_ref[...] = grad[: token_ref.shape[0]].astype(F32)


def regrouped(rows, share):
    channels = rows[0][0].shape[-1]
    source = lax.broadcasted_iota(jnp.int32, (channels, channels), 0)
    target = lax.broadcasted_iota(jnp.int32, (channels, channels), 1)
    core, chip, place = source // share % 2, source // (2 * share), source % share
    moved = core * (channels // 2) + chip * share + place
    select = jnp.where(moved == target, 1.0, 0.0).astype(BF16)
    columns = rows[0][0].shape[0]
    joined = jnp.concatenate([block for row in rows for block in row], axis=0)
    joined = jnp.dot(joined, select, preferred_element_type=F32).astype(BF16)
    frames = len(rows[0])
    return [
        [
            joined[(row * frames + frame) * columns : (row * frames + frame + 1) * columns]
            for frame in range(frames)
        ]
        for row in range(len(rows))
    ]


def split_gradient(store, seams, grad_ref, first_slot, even_ref, odd_ref):
    chips, _, share, channels = even_ref.shape
    rows, frames, _, _ = grad_ref.shape
    half = channels // 2
    grad = grad_ref[...].reshape(-1, channels)
    turned = grad.astype(F32).T.astype(BF16)
    right = []
    for index in range(9):
        cells = side_by_side(store, seams, range(rows), frames, 1, index)
        left = lax.dot_general(cells, grad, (((0,), (0,)), ((), ())), preferred_element_type=F32)
        across = jnp.dot(turned, cells, preferred_element_type=F32)
        for member in range(3):
            first = member * channels
            block = left[first : first + half].reshape(chips, share, channels)
            even_ref[:, first_slot + 3 * index + member] = block.astype(BF16)
            right.append(across[:, first : first + channels])
    even_ref[:, first_slot + TAPS] = jnp.zeros((chips, share, channels), BF16)
    lane = lax.broadcasted_iota(jnp.int32, right[0].shape, 1)
    for pair in range(SLOTS // 2):
        block = pltpu.roll(right[pair], half, 1)
        if pair + SLOTS // 2 < TAPS:
            upper = right[pair + SLOTS // 2]
        else:
            upper = jnp.zeros_like(block)
        block = jnp.where(lane < half, block, upper).reshape(chips, 2, share, channels)
        odd_ref[:, first_slot + 2 * pair] = block[:, 0].astype(BF16)
        odd_ref[:, first_slot + 2 * pair + 1] = block[:, 1].astype(BF16)


def second_kernel_gradient(next_ref, grad_ref, even_ref, odd_ref, token_ref, store):
    rows, share = grad_ref.shape[0], even_ref.shape[2]
    last = at_last_tile()
    seams = {(rows - 3, 2): last, (rows - 2, 0): last}
    window = window_of(regrouped(block_rows(next_ref), share))
    store_columns(store, window, (0, 1, 2), seams)
    split_gradient(store, seams, grad_ref, 0, even_ref, odd_ref)
    token_ref[...] = jnp.zeros_like(token_ref)


def first_kernel_gradient(
    own_ref, earlier_ref, below_ref, grad_ref, even_second, odd_second, keep_ref, send_ref, store,
    even_ref, odd_ref,
):
    rows, share = grad_ref.shape[0], keep_ref.shape[2]
    last = at_last_tile()
    seams = {(rows - 2, 2): last, (rows - 1, 0): last}
    blocks = first_rows((earlier_ref, own_ref), below_ref, rows + 2)
    store_columns(store, window_of(regrouped(blocks, share)), (0, 1, 2), seams)
    split_gradient(store, seams, grad_ref, 0, even_ref, odd_ref)
    odd = lax.axis_index("tile") % 2 == 1

    @pl.when(odd)
    def _():
        keep_ref[:, :SLOTS], keep_ref[:, SLOTS:] = odd_ref[...], odd_second[...]
        send_ref[:, :SLOTS], send_ref[:, SLOTS:] = even_ref[...], even_second[...]

    @pl.when(jnp.logical_not(odd))
    def _():
        keep_ref[:, :SLOTS], keep_ref[:, SLOTS:] = even_ref[...], even_second[...]
        send_ref[:, :SLOTS], send_ref[:, SLOTS:] = odd_ref[...], odd_second[...]


def pack_rows(own_ref, later_ref, token_ref, out_ref):
    del token_ref
    frames, first = own_ref.shape[1], own_ref.shape[0] - out_ref.shape[0]
    out_ref[:, :frames] = own_ref[first:]
    out_ref[:, frames:] = later_ref[first:]


def add_pair(keep_ref, came_ref, out_ref, token_ref):
    out_ref[...] = (keep_ref[...].astype(F32) + came_ref[...].astype(F32)).astype(BF16)
    token_ref[...] = jnp.zeros_like(token_ref)


def sum_first(in_ref, token_ref, out_ref, rows_ref):
    del token_ref
    total = in_ref[0].astype(F32)
    for source in range(1, in_ref.shape[0]):
        total = total + in_ref[source].astype(F32)
    slots, share, channels = total.shape
    groups, width, lanes = out_ref.shape
    rows_ref[...] = jnp.zeros_like(rows_ref)
    odd = lax.axis_index("tile") % 2 == 1

    @pl.when(jnp.logical_not(odd))
    def _():
        stride = lanes // share
        for place in range(share):
            rows_ref[place * stride : place * stride + slots] = total[:, place]
        out_ref[...] = rows_ref[...].T.reshape(groups, width, lanes).astype(BF16)

    @pl.when(odd)
    def _():
        stride = lanes // width
        pairs = total.reshape(slots // 2, 2, share, channels)
        for channel in range(width):
            value = pairs[:, channel // share, channel % share]
            rows_ref[channel * stride : channel * stride + slots // 2] = value
        turned = rows_ref[...].T.reshape(2, groups, share, lanes).astype(BF16)
        for upper in range(2):
            out_ref[:, upper * share : (upper + 1) * share] = turned[upper]


def sum_second(scale, in_ref, out_ref):
    total = in_ref[0].astype(F32)
    for source in range(1, in_ref.shape[0]):
        total = total + in_ref[source].astype(F32)
    total = total * scale
    lanes = total.shape[1]
    share, width, _ = out_ref.shape
    odd = lax.axis_index("tile") % 2 == 1

    @pl.when(jnp.logical_not(odd))
    def _():
        stride = lanes // share
        for place in range(share):
            for layer in range(2):
                start = place * stride + layer * SLOTS
                out_ref[place, :, layer * TAPS : (layer + 1) * TAPS] = total[:, start : start + TAPS]

    @pl.when(odd)
    def _():
        stride, pairs = lanes // width, SLOTS // 2
        for upper in range(2):
            count = TAPS - pairs if upper else pairs
            for layer in range(2):
                first = layer * TAPS + upper * pairs
                for place in range(share):
                    row = upper * share + place
                    for channel in range(width):
                        start = channel * stride + layer * pairs
                        out_ref[place, channel : channel + 1, first : first + count] = total[
                            row : row + 1, start : start + count
                        ]


def shape_of(*dims, dtype=BF16):
    return jax.ShapeDtypeStruct(dims, dtype)


def local(saved_codes, saved_scales, kernels, norm_gains, cotangent):
    frames, rows, columns, channels = saved_codes.shape
    tiles, groups = lax.axis_size("tile"), lax.axis_size("frame")
    cells = frames * rows * columns
    block = (columns, channels)

    def column_store(window_rows, window_frames):
        return (pltpu.VMEM((window_rows + 2, window_frames, columns, 3 * channels), BF16),)

    def next_frames(value, steps):
        return lax.ppermute(value, "frame", [(i, i + steps) for i in range(groups - steps)])

    def earlier_frames(value):
        return lax.ppermute(value, "frame", [(i + 1, i) for i in range(groups - 1)])

    def from_below(value):
        return lax.ppermute(value, "tile", [((i + 1) % tiles, i) for i in range(tiles)])

    def from_above(value):
        return lax.ppermute(value, "tile", [(i, (i + 1) % tiles) for i in range(tiles)])

    def partner(value):
        return lax.ppermute(value, "tile", [(i, i ^ 1) for i in range(tiles)])

    own_0 = (saved_codes.astype(F32) * saved_scales[..., None]).astype(BF16)
    earlier_0, earliest_0 = next_frames(own_0, 1), next_frames(own_0, 2)
    sent = jnp.concatenate(
        [
            earliest_0.reshape(frames * rows, *block),
            earlier_0.reshape(frames * rows, *block),
            own_0.reshape(frames * rows, *block),
            cotangent[:, :2].reshape(frames * 2, *block),
        ],
        axis=0,
    )
    below = from_below(sent)
    wide = 2 * rows - 2
    grad_shape = shape_of(rows, frames, *block)
    next_1, pre_0, grad_1 = call(
        forward,
        (shape_of(wide, 2 * frames, *block), shape_of(cells, channels, dtype=F32), grad_shape),
        own_0,
        earlier_0,
        earliest_0,
        below,
        cotangent,
        kernels[0],
        kernels[1],
        norm_gains,
        scratch=column_store(2 * rows, 3 * frames) + column_store(wide, 2 * frames),
    )

    share = channels // tiles
    part = shape_of(tiles // 2, SLOTS, share, channels)
    both = shape_of(tiles // 2, 2 * SLOTS, share, channels)
    mark = shape_of(8, channels, dtype=F32)

    def with_neighbours(later, grad, token):
        edge = shape_of(2, 2 * frames, *block)
        packed = call(pack_rows, edge, grad, later, token)
        return from_above(packed)

    chips = [[f * tiles + t for t in range(0, tiles, 2)] for f in range(groups)]
    odd_chips = [[f * tiles + t for t in range(1, tiles, 2)] for f in range(groups)]
    even_frames = [[f * tiles + t for f in range(groups)] for t in range(0, tiles, 2)]
    odd_frames = [[f * tiles + t for f in range(groups)] for t in range(1, tiles, 2)]

    def exchanged(value, members):
        return lax.all_to_all(
            value, ("frame", "tile"), 0, 0, tiled=True, axis_index_groups=members
        )

    later_1 = earlier_frames(grad_1)
    even_1, odd_1, token = call(
        second_kernel_gradient,
        (part, part, mark),
        next_1,
        grad_1,
        scratch=column_store(wide, 2 * frames),
    )
    above_1 = with_neighbours(later_1, grad_1, token)
    grad_0 = call(
        second_backward,
        grad_shape,
        grad_1,
        later_1,
        above_1,
        kernels[1],
        norm_gains,
        pre_0,
        scratch=column_store(rows + 2, 2 * frames),
    )
    keep, send = call(
        first_kernel_gradient,
        (both, both),
        own_0,
        earlier_0,
        below,
        grad_0,
        even_1,
        odd_1,
        scratch=column_store(rows + 2, 2 * frames)
        + (pltpu.VMEM(part.shape, BF16), pltpu.VMEM(part.shape, BF16)),
    )
    paired, token = call(add_pair, (both, mark), keep, partner(send))
    arrived = exchanged(paired, chips + odd_frames)
    later_0 = earlier_frames(grad_0)
    above_0 = with_neighbours(later_0, grad_0, token)
    input_grad, token = call(
        first_backward,
        (shape_of(frames, rows, *block), mark),
        grad_0,
        later_0,
        above_0,
        kernels[0],
        scratch=column_store(rows + 2, 2 * frames),
    )
    lanes = share * 64
    halfway = call(
        sum_first,
        shape_of(groups, channels // groups, lanes),
        arrived,
        token,
        scratch=(pltpu.VMEM((lanes, channels), F32),),
    )
    spread = exchanged(halfway, even_frames + odd_chips)
    scale = 1.0 / math.sqrt(cells * tiles * groups)
    summed = call(
        lambda *refs: sum_second(scale, *refs),
        shape_of(share, channels // groups, 2 * TAPS, dtype=F32),
        spread,
    )
    return (input_grad, jnp.transpose(summed, (2, 0, 1)))


def solution(mesh):
    in_specs = (
        P("frame", "tile", None, None),
        P("frame", "tile", None),
        P(),
        P(),
        P("frame", "tile", None, None),
    )
    out_specs = (P("frame", "tile", None, None), P(None, "tile", "frame"))

    return jax.shard_map(local, mesh=mesh, in_specs=in_specs, out_specs=out_specs, check_vma=False)
```

```python
import math

import jax
import jax.numpy as jnp
from jax import lax
from jax.experimental import pallas as pl
from jax.experimental.pallas import tpu as pltpu
from jax.sharding import PartitionSpec as P


EPS = 1e-06
TAPS = 27
F32 = jnp.float32
BF16 = jnp.bfloat16


def call(kernel, out_shape, *operands, scratch=()):
    return pl.pallas_call(
        kernel,
        out_shape=out_shape,
        scratch_shapes=list(scratch),
        compiler_params=pltpu.CompilerParams(vmem_limit_bytes=48 * 2**20),
    )(*operands)


def shifted_columns(block):
    shape = block.shape
    columns = shape[-2]
    flat = block.astype(F32).reshape(-1, shape[-1])
    column = lax.broadcasted_iota(jnp.int32, flat.shape, 0) % columns
    before = jnp.where(column == 0, 0.0, pltpu.roll(flat, 1, 0))
    after = jnp.where(column == columns - 1, 0.0, pltpu.roll(flat, flat.shape[0] - 1, 0))
    return before.astype(BF16).reshape(shape), block, after.astype(BF16).reshape(shape)


def store_columns(store, window, order, seams):
    for row, blocks in enumerate(window):
        for frame, triple in enumerate(blocks):
            store[row, frame] = jnp.concatenate([triple[across] for across in order], axis=1)
    for extra, ((row, offset), seam) in enumerate(seams.items()):
        for frame in range(store.shape[1]):
            source = store[row + offset, frame]
            store[len(window) + extra, frame] = jnp.where(seam, jnp.zeros_like(source), source)


def side_by_side(store, seams, rows, frames, sign, index):
    depth, down = divmod(index, 3)
    if sign < 0:
        depth, down = 2 - depth, 2 - down
    extra, total = list(seams), store.shape[0] - len(seams)
    pieces = []
    for row in rows:
        place = total + extra.index((row, down)) if (row, down) in seams else row + down
        pieces.append(store[place, depth : depth + frames].reshape(-1, store.shape[-1]))
    return jnp.concatenate(pieces, axis=0)


def product(store, seams, rows, frames, sign, kernel_ref):
    total = None
    for index in range(0, 9, 2):
        members = range(index, min(index + 2, 9))
        cells = jnp.concatenate(
            [side_by_side(store, seams, rows, frames, sign, member) for member in members], axis=1
        )
        taps = range(3 * members[0], 3 * members[-1] + 3)
        if sign > 0:
            weights = kernel_ref[taps[0] : taps[-1] + 1].reshape(-1, kernel_ref.shape[-1])
            part = jnp.dot(cells, weights, preferred_element_type=F32)
        else:
            weights = jnp.concatenate([kernel_ref[tap] for tap in taps], axis=1)
            part = lax.dot_general(
                cells, weights, (((1,), (1,)), ((), ())), preferred_element_type=F32
            )
        total = part if total is None else total + part
    return total


def window_of(rows):
    return [[shifted_columns(block) for block in row] for row in rows]


def block_rows(ref):
    return [[ref[row, frame] for frame in range(ref.shape[1])] for row in range(ref.shape[0])]


def silu_parts(pre_norm, gain):
    inverse = lax.rsqrt(jnp.mean(pre_norm * pre_norm, axis=-1, keepdims=True) + EPS)
    normed = pre_norm * inverse * gain
    return inverse, normed, 1.0 / (1.0 + jnp.exp(-normed))


def pre_norm_gradient(pre_norm, gain, upstream):
    inverse, normed, sigma = silu_parts(pre_norm, gain)
    scaled = gain * upstream * sigma * (1.0 + normed * (1.0 - sigma))
    mixed = jnp.mean(pre_norm * scaled, axis=-1, keepdims=True)
    return (inverse * scaled - pre_norm * inverse**3 * mixed).astype(BF16)


def at_last_tile():
    return lax.axis_index("tile") == lax.axis_size("tile") - 1


def first_rows(parts, below_parts, total):
    frames, rows = parts[0].shape[:2]
    result = []
    for row in range(total):
        source, place = (parts, row) if row < rows else (below_parts, row - rows)
        result.append([part[frame, place] for part in source for frame in range(frames)])
    return result


def forward(
    own_ref, earlier_ref, earliest_ref, below_ref, below_earlier_ref, below_earliest_ref, top_ref,
    first_kernel_ref, second_kernel_ref, gain_ref, next_ref, pre_ref, grad_ref, wide_store, store,
):
    frames, rows, columns, _ = own_ref.shape
    last = at_last_tile()
    window = window_of(
        first_rows(
            (earliest_ref, earlier_ref, own_ref),
            (below_earliest_ref, below_earlier_ref, below_ref),
            2 * rows,
        )
    )
    wide, deep = 2 * rows - 2, 2 * frames
    seams = {(rows - 2, 2): last, (rows - 1, 0): last}
    store_columns(wide_store, window, (0, 1, 2), seams)
    own_cells = frames * columns
    for first in range(0, wide, 2):
        pre_norm = product(wide_store, seams, (first, first + 1), deep, 1, first_kernel_ref)
        _, normed, sigma = silu_parts(pre_norm, gain_ref[0:1])
        value = (normed * sigma).astype(BF16)
        for block in range(2 * deep):
            row, frame = first + block // deep, block % deep
            cells = slice(block * columns, (block + 1) * columns)
            next_ref[row, frame] = value[cells]
            if row < rows and frame >= frames:
                start = row * own_cells + (frame - frames) * columns
                pre_ref[start : start + columns] = pre_norm[cells]
    seams = {(rows - 3, 2): last, (rows - 2, 0): last}
    store_columns(store, window_of(block_rows(next_ref)), (0, 1, 2), seams)
    pre_norm = product(store, seams, range(rows), frames, 1, second_kernel_ref)
    spread = []
    for row in range(rows):
        for frame in range(frames):
            if row < rows - 2:
                spread.append(top_ref[frame, row + 2])
            else:
                spread.append(below_ref[frame, row + 2])
    upstream = jnp.concatenate(spread, axis=0).astype(F32)
    grad_ref[...] = pre_norm_gradient(pre_norm, gain_ref[1:2], upstream).reshape(grad_ref.shape)


def backward_rows(own_ref, later_ref, above_ref, corner_ref):
    window = []
    for near_ref, far_ref in ((above_ref, corner_ref), (own_ref, later_ref)):
        window += [near + far for near, far in zip(block_rows(near_ref), block_rows(far_ref))]
    return window


def second_backward(
    own_ref, later_ref, above_ref, corner_ref, kernel_ref, gain_ref, pre_ref, grad_ref, store
):
    rows, frames, _, _ = own_ref.shape
    last = at_last_tile()
    seams = {(rows - 2, 2): last, (rows - 1, 0): last}
    window = window_of(backward_rows(own_ref, later_ref, above_ref, corner_ref))
    store_columns(store, window, (2, 1, 0), seams)
    upstream = product(store, seams, range(rows), frames, -1, kernel_ref).astype(BF16).astype(F32)
    grad_ref[...] = pre_norm_gradient(pre_ref[...], gain_ref[0:1], upstream).reshape(grad_ref.shape)


def first_backward(
    own_ref, later_ref, above_ref, corner_ref, kernel_ref, out_ref, token_ref, store
):
    rows, frames, columns, _ = own_ref.shape
    seams = {(0, 0): lax.axis_index("tile") == 0, (rows - 1, 2): at_last_tile()}
    window = window_of(backward_rows(own_ref, later_ref, above_ref, corner_ref))
    store_columns(store, window, (2, 1, 0), seams)
    grad = product(store, seams, range(rows), frames, -1, kernel_ref).astype(BF16)
    for row in range(rows):
        for frame in range(frames):
            cell = (row * frames + frame) * columns
            out_ref[frame, row] = grad[cell : cell + columns]
    token_ref[...] = grad[: token_ref.shape[0]].astype(F32)


def split_gradient(store, seams, grad_ref, keep_ref, send_ref):
    chips, _, share, channels = keep_ref.shape
    rows, frames, _, _ = grad_ref.shape
    odd = lax.axis_index("tile") % 2 == 1
    grad = grad_ref[...].reshape(-1, channels)
    for index in range(9):
        blocks = lax.dot_general(
            side_by_side(store, seams, range(rows), frames, 1, index),
            grad,
            (((0,), (0,)), ((), ())),
            preferred_element_type=F32,
        )
        for across in range(3):
            block = blocks[across * channels : (across + 1) * channels]
            block = block.reshape(chips, 2, share, channels)
            even_part, odd_part = block[:, 0], block[:, 1]
            tap = 3 * index + across
            keep_ref[:, tap] = jnp.where(odd, odd_part, even_part).astype(BF16)
            send_ref[:, tap] = jnp.where(odd, even_part, odd_part).astype(BF16)


def second_kernel_gradient(next_ref, grad_ref, keep_ref, send_ref, store):
    rows = grad_ref.shape[0]
    last = at_last_tile()
    seams = {(rows - 3, 2): last, (rows - 2, 0): last}
    store_columns(store, window_of(block_rows(next_ref)), (0, 1, 2), seams)
    split_gradient(store, seams, grad_ref, keep_ref, send_ref)


def first_kernel_gradient(
    own_ref, earlier_ref, below_ref, below_earlier_ref, grad_ref, keep_second, send_second,
    keep_ref, send_ref, store,
):
    rows = grad_ref.shape[0]
    last = at_last_tile()
    seams = {(rows - 2, 2): last, (rows - 1, 0): last}
    window = window_of(
        first_rows((earlier_ref, own_ref), (below_earlier_ref, below_ref), rows + 2)
    )
    store_columns(store, window, (0, 1, 2), seams)
    keep_ref[:, TAPS:], send_ref[:, TAPS:] = keep_second[...], send_second[...]
    split_gradient(store, seams, grad_ref, keep_ref, send_ref)


def add_pair(keep_ref, came_ref, out_ref):
    out_ref[...] = (keep_ref[...].astype(F32) + came_ref[...].astype(F32)).astype(BF16)


def sum_tiles(in_ref, token_ref, out_ref, rows_ref):
    del token_ref
    total = in_ref[0].astype(F32)
    for chip in range(1, in_ref.shape[0]):
        total = total + in_ref[chip].astype(F32)
    taps, share, _ = total.shape
    groups, width, lanes = out_ref.shape
    stride = lanes // share
    rows_ref[...] = jnp.zeros_like(rows_ref)
    for place in range(share):
        rows_ref[place * stride : place * stride + taps] = total[:, place]
    out_ref[...] = rows_ref[...].T.reshape(groups, width, lanes).astype(BF16)


def sum_frames(scale, in_ref, out_ref):
    total = in_ref[0].astype(F32)
    for group in range(1, in_ref.shape[0]):
        total = total + in_ref[group].astype(F32)
    share, _, taps = out_ref.shape
    stride = total.shape[1] // share
    for place in range(share):
        out_ref[place] = total[:, place * stride : place * stride + taps] * scale


def shape_of(*dims, dtype=BF16):
    return jax.ShapeDtypeStruct(dims, dtype)


def local(saved_codes, saved_scales, kernels, norm_gains, cotangent):
    frames, rows, columns, channels = saved_codes.shape
    tiles, groups = lax.axis_size("tile"), lax.axis_size("frame")
    cells = frames * rows * columns
    block = (columns, channels)

    def column_store(window_rows, window_frames):
        return (pltpu.VMEM((window_rows + 2, window_frames, columns, 3 * channels), BF16),)

    def moved(value, frame_steps, tile_steps):
        pairs = [
            (f * tiles + t, (f + frame_steps) * tiles + (t + tile_steps) % tiles)
            for f in range(groups)
            for t in range(tiles)
            if 0 <= f + frame_steps < groups
        ]
        return lax.ppermute(value, ("frame", "tile"), pairs)

    own_0 = (saved_codes.astype(F32) * saved_scales[..., None]).astype(BF16)
    earliest_0, below_earliest = moved(own_0, 2, 0), moved(own_0, 2, -1)
    earlier_0, below_earlier = moved(own_0, 1, 0), moved(own_0, 1, -1)
    below = moved(jnp.concatenate([own_0, cotangent[:, :2]], axis=1), 0, -1)
    wide = 2 * rows - 2
    grad_shape = shape_of(rows, frames, *block)
    next_1, pre_0, grad_1 = call(
        forward,
        (shape_of(wide, 2 * frames, *block), shape_of(cells, channels, dtype=F32), grad_shape),
        own_0,
        earlier_0,
        earliest_0,
        below,
        below_earlier,
        below_earliest,
        cotangent,
        kernels[0],
        kernels[1],
        norm_gains,
        scratch=column_store(2 * rows, 3 * frames) + column_store(wide, 2 * frames),
    )

    def neighbours(grad):
        edge = grad[rows - 2 :]
        later = moved(grad, -1, 0)
        corner = moved(edge, -1, 1)
        above = moved(edge, 0, 1)
        return later, above, corner

    share = channels // tiles
    part = shape_of(tiles // 2, TAPS, share, channels)
    both = shape_of(tiles // 2, 2 * TAPS, share, channels)
    mark = shape_of(8, channels, dtype=F32)
    next_to = neighbours(grad_1)
    keep_1, send_1 = call(
        second_kernel_gradient,
        (part, part),
        next_1,
        grad_1,
        scratch=column_store(wide, 2 * frames),
    )
    grad_0 = call(
        second_backward,
        grad_shape,
        grad_1,
        *next_to,
        kernels[1],
        norm_gains,
        pre_0,
        scratch=column_store(rows + 2, 2 * frames),
    )
    keep, send = call(
        first_kernel_gradient,
        (both, both),
        own_0,
        earlier_0,
        below,
        below_earlier,
        grad_0,
        keep_1,
        send_1,
        scratch=column_store(rows + 2, 2 * frames),
    )
    came = lax.ppermute(send, "tile", [(i, i ^ 1) for i in range(tiles)])
    paired = call(add_pair, both, keep, came)
    by_core = [list(range(core, tiles, 2)) for core in range(2)]
    arrived = lax.all_to_all(paired, "tile", 0, 0, tiled=True, axis_index_groups=by_core)
    next_to = neighbours(grad_0)
    input_grad, token = call(
        first_backward,
        (shape_of(frames, rows, *block), mark),
        grad_0,
        *next_to,
        kernels[0],
        scratch=column_store(rows + 2, 2 * frames),
    )
    lanes = 64 * share
    by_frame = call(
        sum_tiles,
        shape_of(groups, channels // groups, lanes),
        arrived,
        token,
        scratch=(pltpu.VMEM((lanes, channels), F32),),
    )
    spread = lax.all_to_all(by_frame, "frame", 0, 0, tiled=True)
    scale = 1.0 / math.sqrt(cells * tiles * groups)
    summed = call(
        lambda *refs: sum_frames(scale, *refs),
        shape_of(share, channels // groups, 2 * TAPS, dtype=F32),
        spread,
    )
    return (input_grad, jnp.transpose(summed, (2, 0, 1)))


def solution(mesh):
    in_specs = (
        P("frame", "tile", None, None),
        P("frame", "tile", None),
        P(),
        P(),
        P("frame", "tile", None, None),
    )
    out_specs = (P("frame", "tile", None, None), P(None, "tile", "frame"))

    return jax.shard_map(local, mesh=mesh, in_specs=in_specs, out_specs=out_specs, check_vma=False)
```

```python
import math

import jax
import jax.numpy as jnp
from jax import lax
from jax.experimental import pallas as pl
from jax.experimental.pallas import tpu as pltpu
from jax.sharding import PartitionSpec as P


EPS = 1e-06
TAPS = 27
F32 = jnp.float32
BF16 = jnp.bfloat16


def call(kernel, out_shape, *operands, scratch=()):
    return pl.pallas_call(
        kernel,
        out_shape=out_shape,
        scratch_shapes=list(scratch),
        compiler_params=pltpu.CompilerParams(vmem_limit_bytes=48 * 2**20),
    )(*operands)


def shifted_columns(block):
    shape = block.shape
    columns = shape[-2]
    flat = block.astype(F32).reshape(-1, shape[-1])
    column = lax.broadcasted_iota(jnp.int32, flat.shape, 0) % columns
    before = jnp.where(column == 0, 0.0, pltpu.roll(flat, 1, 0))
    after = jnp.where(column == columns - 1, 0.0, pltpu.roll(flat, flat.shape[0] - 1, 0))
    return before.astype(BF16).reshape(shape), block, after.astype(BF16).reshape(shape)


def store_columns(store, window, order, seams):
    for row, blocks in enumerate(window):
        for frame, triple in enumerate(blocks):
            store[row, frame] = jnp.concatenate([triple[across] for across in order], axis=1)
    for extra, ((row, offset), seam) in enumerate(seams.items()):
        for frame in range(store.shape[1]):
            source = store[row + offset, frame]
            store[len(window) + extra, frame] = jnp.where(seam, jnp.zeros_like(source), source)


def side_by_side(store, seams, rows, frames, sign, index):
    depth, down = divmod(index, 3)
    if sign < 0:
        depth, down = 2 - depth, 2 - down
    extra, total = list(seams), store.shape[0] - len(seams)
    pieces = []
    for row in rows:
        place = total + extra.index((row, down)) if (row, down) in seams else row + down
        pieces.append(store[place, depth : depth + frames].reshape(-1, store.shape[-1]))
    return jnp.concatenate(pieces, axis=0)


def product(store, seams, rows, frames, sign, kernel_ref):
    total = None
    for index in range(0, 9, 2):
        members = range(index, min(index + 2, 9))
        cells = jnp.concatenate(
            [side_by_side(store, seams, rows, frames, sign, member) for member in members], axis=1
        )
        taps = range(3 * members[0], 3 * members[-1] + 3)
        if sign > 0:
            weights = kernel_ref[taps[0] : taps[-1] + 1].reshape(-1, kernel_ref.shape[-1])
            part = jnp.dot(cells, weights, preferred_element_type=F32)
        else:
            weights = jnp.concatenate([kernel_ref[tap] for tap in taps], axis=1)
            part = lax.dot_general(
                cells, weights, (((1,), (1,)), ((), ())), preferred_element_type=F32
            )
        total = part if total is None else total + part
    return total


def window_of(rows):
    return [[shifted_columns(block) for block in row] for row in rows]


def block_rows(ref):
    return [[ref[row, frame] for frame in range(ref.shape[1])] for row in range(ref.shape[0])]


def silu_parts(pre_norm, gain):
    inverse = lax.rsqrt(jnp.mean(pre_norm * pre_norm, axis=-1, keepdims=True) + EPS)
    normed = pre_norm * inverse * gain
    return inverse, normed, 1.0 / (1.0 + jnp.exp(-normed))


def pre_norm_gradient(pre_norm, gain, upstream):
    inverse, normed, sigma = silu_parts(pre_norm, gain)
    scaled = gain * upstream * sigma * (1.0 + normed * (1.0 - sigma))
    mixed = jnp.mean(pre_norm * scaled, axis=-1, keepdims=True)
    return (inverse * scaled - pre_norm * inverse**3 * mixed).astype(BF16)


def at_last_tile():
    return lax.axis_index("tile") == lax.axis_size("tile") - 1


def first_rows(parts, below_ref, total):
    frames, rows = parts[0].shape[:2]
    skipped = (3 - len(parts)) * frames
    result = []
    for row in range(total):
        if row < rows:
            result.append([part[frame, row] for part in parts for frame in range(frames)])
        else:
            result.append(
                [
                    below_ref[(skipped + frame) * rows + row - rows]
                    for frame in range(len(parts) * frames)
                ]
            )
    return result


def forward(
    own_ref, earlier_ref, earliest_ref, below_ref, top_ref, first_kernel_ref, second_kernel_ref,
    gain_ref, next_ref, pre_ref, grad_ref, wide_store, store,
):
    frames, rows, columns, _ = own_ref.shape
    last = at_last_tile()
    window = window_of(first_rows((earliest_ref, earlier_ref, own_ref), below_ref, 2 * rows))
    wide, deep = 2 * rows - 2, 2 * frames
    seams = {(rows - 2, 2): last, (rows - 1, 0): last}
    store_columns(wide_store, window, (0, 1, 2), seams)
    own_cells = frames * columns
    for first in range(0, wide, 2):
        pre_norm = product(wide_store, seams, (first, first + 1), deep, 1, first_kernel_ref)
        _, normed, sigma = silu_parts(pre_norm, gain_ref[0:1])
        value = (normed * sigma).astype(BF16)
        for block in range(2 * deep):
            row, frame = first + block // deep, block % deep
            cells = slice(block * columns, (block + 1) * columns)
            next_ref[row, frame] = value[cells]
            if row < rows and frame >= frames:
                start = row * own_cells + (frame - frames) * columns
                pre_ref[start : start + columns] = pre_norm[cells]
    seams = {(rows - 3, 2): last, (rows - 2, 0): last}
    store_columns(store, window_of(block_rows(next_ref)), (0, 1, 2), seams)
    pre_norm = product(store, seams, range(rows), frames, 1, second_kernel_ref)
    spread = []
    for row in range(rows):
        for frame in range(frames):
            if row < rows - 2:
                spread.append(top_ref[frame, row + 2])
            else:
                spread.append(below_ref[3 * frames * rows + frame * 2 + row - rows + 2])
    upstream = jnp.concatenate(spread, axis=0).astype(F32)
    grad_ref[...] = pre_norm_gradient(pre_norm, gain_ref[1:2], upstream).reshape(grad_ref.shape)


def backward_rows(own_ref, later_ref, above_ref, frames):
    rows = own_ref.shape[0]
    result = []
    for row in range(2):
        result.append([above_ref[row, frame] for frame in range(2 * frames)])
    for row in range(rows):
        result.append(
            [own_ref[row, frame] for frame in range(frames)]
            + [later_ref[row, frame] for frame in range(frames)]
        )
    return result


def second_backward(
    own_ref, later_ref, above_ref, kernel_ref, gain_ref, pre_ref, grad_ref, store
):
    rows, frames, _, _ = own_ref.shape
    last = at_last_tile()
    seams = {(rows - 2, 2): last, (rows - 1, 0): last}
    window = window_of(backward_rows(own_ref, later_ref, above_ref, frames))
    store_columns(store, window, (2, 1, 0), seams)
    upstream = product(store, seams, range(rows), frames, -1, kernel_ref).astype(BF16).astype(F32)
    grad_ref[...] = pre_norm_gradient(pre_ref[...], gain_ref[0:1], upstream).reshape(grad_ref.shape)


def first_backward(own_ref, later_ref, above_ref, kernel_ref, out_ref, token_ref, store):
    rows, frames, columns, _ = own_ref.shape
    seams = {(0, 0): lax.axis_index("tile") == 0, (rows - 1, 2): at_last_tile()}
    window = window_of(backward_rows(own_ref, later_ref, above_ref, frames))
    store_columns(store, window, (2, 1, 0), seams)
    grad = product(store, seams, range(rows), frames, -1, kernel_ref).astype(BF16)
    for row in range(rows):
        for frame in range(frames):
            cell = (row * frames + frame) * columns
            out_ref[frame, row] = grad[cell : cell + columns]
    token_ref[...] = grad[: token_ref.shape[0]].astype(F32)


def split_gradient(store, seams, grad_ref, keep_ref, send_ref):
    chips, _, share, channels = keep_ref.shape
    rows, frames, _, _ = grad_ref.shape
    odd = lax.axis_index("tile") % 2 == 1
    grad = grad_ref[...].reshape(-1, channels)
    for index in range(9):
        blocks = lax.dot_general(
            side_by_side(store, seams, range(rows), frames, 1, index),
            grad,
            (((0,), (0,)), ((), ())),
            preferred_element_type=F32,
        )
        for across in range(3):
            block = blocks[across * channels : (across + 1) * channels]
            block = block.reshape(chips, 2, share, channels)
            even_part, odd_part = block[:, 0], block[:, 1]
            tap = 3 * index + across
            keep_ref[:, tap] = jnp.where(odd, odd_part, even_part).astype(BF16)
            send_ref[:, tap] = jnp.where(odd, even_part, odd_part).astype(BF16)


def second_kernel_gradient(next_ref, grad_ref, keep_ref, send_ref, store):
    rows = grad_ref.shape[0]
    last = at_last_tile()
    seams = {(rows - 3, 2): last, (rows - 2, 0): last}
    store_columns(store, window_of(block_rows(next_ref)), (0, 1, 2), seams)
    split_gradient(store, seams, grad_ref, keep_ref, send_ref)


def first_kernel_gradient(
    own_ref, earlier_ref, below_ref, grad_ref, keep_second, send_second, keep_ref, send_ref, store
):
    rows = grad_ref.shape[0]
    last = at_last_tile()
    seams = {(rows - 2, 2): last, (rows - 1, 0): last}
    window = window_of(first_rows((earlier_ref, own_ref), below_ref, rows + 2))
    store_columns(store, window, (0, 1, 2), seams)
    keep_ref[:, TAPS:], send_ref[:, TAPS:] = keep_second[...], send_second[...]
    split_gradient(store, seams, grad_ref, keep_ref, send_ref)


def pack_rows(own_ref, later_ref, out_ref):
    frames, first = own_ref.shape[1], own_ref.shape[0] - out_ref.shape[0]
    out_ref[:, :frames] = own_ref[first:]
    out_ref[:, frames:] = later_ref[first:]


def add_pair(keep_ref, came_ref, out_ref):
    out_ref[...] = (keep_ref[...].astype(F32) + came_ref[...].astype(F32)).astype(BF16)


def sum_tiles(share, in_ref, token_ref, out_ref, rows_ref):
    del token_ref
    total = in_ref[0].astype(F32)
    for chip in range(1, in_ref.shape[0]):
        total = total + in_ref[chip].astype(F32)
    groups, width, lanes = out_ref.shape
    stride, taps = lanes // share, 2 * TAPS
    total = total.reshape(taps, share, -1)
    rows_ref[...] = jnp.zeros_like(rows_ref)
    for place in range(share):
        rows_ref[place * stride : place * stride + taps] = total[:, place]
    out_ref[...] = rows_ref[...].T.reshape(groups, width, lanes).astype(BF16)


def sum_frames(scale, in_ref, out_ref):
    total = in_ref[0].astype(F32)
    for group in range(1, in_ref.shape[0]):
        total = total + in_ref[group].astype(F32)
    share, _, taps = out_ref.shape
    stride = total.shape[1] // share
    for place in range(share):
        out_ref[place] = total[:, place * stride : place * stride + taps] * scale


def shape_of(*dims, dtype=BF16):
    return jax.ShapeDtypeStruct(dims, dtype)


def local(saved_codes, saved_scales, kernels, norm_gains, cotangent):
    frames, rows, columns, channels = saved_codes.shape
    tiles, groups = lax.axis_size("tile"), lax.axis_size("frame")
    cells = frames * rows * columns
    block = (columns, channels)

    def column_store(window_rows, window_frames):
        return (pltpu.VMEM((window_rows + 2, window_frames, columns, 3 * channels), BF16),)

    def next_frames(value, steps):
        return lax.ppermute(value, "frame", [(i, i + steps) for i in range(groups - steps)])

    def earlier_frames(value):
        return lax.ppermute(value, "frame", [(i + 1, i) for i in range(groups - 1)])

    def from_below(value):
        return lax.ppermute(value, "tile", [((i + 1) % tiles, i) for i in range(tiles)])

    def from_above(value):
        return lax.ppermute(value, "tile", [(i, (i + 1) % tiles) for i in range(tiles)])

    def partner(value):
        return lax.ppermute(value, "tile", [(i, i ^ 1) for i in range(tiles)])

    own_0 = (saved_codes.astype(F32) * saved_scales[..., None]).astype(BF16)
    earlier_0, earliest_0 = next_frames(own_0, 1), next_frames(own_0, 2)
    sent = jnp.concatenate(
        [
            earliest_0.reshape(frames * rows, *block),
            earlier_0.reshape(frames * rows, *block),
            own_0.reshape(frames * rows, *block),
            cotangent[:, :2].reshape(frames * 2, *block),
        ],
        axis=0,
    )
    below = from_below(sent)
    wide = 2 * rows - 2
    grad_shape = shape_of(rows, frames, *block)
    next_1, pre_0, grad_1 = call(
        forward,
        (shape_of(wide, 2 * frames, *block), shape_of(cells, channels, dtype=F32), grad_shape),
        own_0,
        earlier_0,
        earliest_0,
        below,
        cotangent,
        kernels[0],
        kernels[1],
        norm_gains,
        scratch=column_store(2 * rows, 3 * frames) + column_store(wide, 2 * frames),
    )

    share = channels // tiles
    part = shape_of(tiles // 2, TAPS, share, channels)
    both = shape_of(tiles // 2, 2 * TAPS, share, channels)
    mark = shape_of(8, channels, dtype=F32)

    def neighbours(grad):
        later = earlier_frames(grad)
        packed = call(pack_rows, shape_of(2, 2 * frames, *block), grad, later)
        return later, from_above(packed)

    next_to = neighbours(grad_1)
    keep_1, send_1 = call(
        second_kernel_gradient,
        (part, part),
        next_1,
        grad_1,
        scratch=column_store(wide, 2 * frames),
    )
    grad_0 = call(
        second_backward,
        grad_shape,
        grad_1,
        *next_to,
        kernels[1],
        norm_gains,
        pre_0,
        scratch=column_store(rows + 2, 2 * frames),
    )
    keep, send = call(
        first_kernel_gradient,
        (both, both),
        own_0,
        earlier_0,
        below,
        grad_0,
        keep_1,
        send_1,
        scratch=column_store(rows + 2, 2 * frames),
    )
    full = shape_of(tiles // 2, 2 * TAPS * share, channels)
    came = partner(send).reshape(full.shape)
    paired = call(add_pair, full, keep.reshape(full.shape), came)
    by_core = [list(range(core, tiles, 2)) for core in range(2)]
    arrived = lax.all_to_all(paired, "tile", 0, 0, tiled=True, axis_index_groups=by_core)
    next_to = neighbours(grad_0)
    input_grad, token = call(
        first_backward,
        (shape_of(frames, rows, *block), mark),
        grad_0,
        *next_to,
        kernels[0],
        scratch=column_store(rows + 2, 2 * frames),
    )
    lanes = 64 * share
    by_frame = call(
        lambda *refs: sum_tiles(share, *refs),
        shape_of(groups, channels // groups, lanes),
        arrived,
        token,
        scratch=(pltpu.VMEM((lanes, channels), F32),),
    )
    spread = lax.all_to_all(by_frame, "frame", 0, 0, tiled=True)
    scale = 1.0 / math.sqrt(cells * tiles * groups)
    summed = call(
        lambda *refs: sum_frames(scale, *refs),
        shape_of(share, channels // groups, 2 * TAPS, dtype=F32),
        spread,
    )
    return (input_grad, jnp.transpose(summed, (2, 0, 1)))


def solution(mesh):
    in_specs = (
        P("frame", "tile", None, None),
        P("frame", "tile", None),
        P(),
        P(),
        P("frame", "tile", None, None),
    )
    out_specs = (P("frame", "tile", None, None), P(None, "tile", "frame"))

    return jax.shard_map(local, mesh=mesh, in_specs=in_specs, out_specs=out_specs, check_vma=False)
```

```python
import math

import jax
import jax.numpy as jnp
from jax import lax
from jax.experimental import pallas as pl
from jax.experimental.pallas import tpu as pltpu
from jax.sharding import PartitionSpec as P


EPS = 1e-06
TAPS = 27
F32 = jnp.float32
BF16 = jnp.bfloat16


def call(kernel, out_shape, *operands, scratch=()):
    return pl.pallas_call(
        kernel,
        out_shape=out_shape,
        scratch_shapes=list(scratch),
        compiler_params=pltpu.CompilerParams(vmem_limit_bytes=48 * 2**20),
    )(*operands)


def shifted_columns(block):
    shape = block.shape
    columns = shape[-2]
    flat = block.astype(F32).reshape(-1, shape[-1])
    column = lax.broadcasted_iota(jnp.int32, flat.shape, 0) % columns
    before = jnp.where(column == 0, 0.0, pltpu.roll(flat, 1, 0))
    after = jnp.where(column == columns - 1, 0.0, pltpu.roll(flat, flat.shape[0] - 1, 0))
    return before.astype(BF16).reshape(shape), block, after.astype(BF16).reshape(shape)


def store_columns(store, window, order, seams):
    for row, blocks in enumerate(window):
        for frame, triple in enumerate(blocks):
            store[row, frame] = jnp.concatenate([triple[across] for across in order], axis=1)
    for extra, ((row, offset), seam) in enumerate(seams.items()):
        for frame in range(store.shape[1]):
            source = store[row + offset, frame]
            store[len(window) + extra, frame] = jnp.where(seam, jnp.zeros_like(source), source)


def side_by_side(store, seams, rows, frames, sign, index):
    depth, down = divmod(index, 3)
    if sign < 0:
        depth, down = 2 - depth, 2 - down
    extra, total = list(seams), store.shape[0] - len(seams)
    pieces = []
    for row in rows:
        place = total + extra.index((row, down)) if (row, down) in seams else row + down
        pieces.append(store[place, depth : depth + frames].reshape(-1, store.shape[-1]))
    return jnp.concatenate(pieces, axis=0)


def product(store, seams, rows, frames, sign, kernel_ref):
    total = None
    for index in range(0, 9, 2):
        members = range(index, min(index + 2, 9))
        cells = jnp.concatenate(
            [side_by_side(store, seams, rows, frames, sign, member) for member in members], axis=1
        )
        taps = range(3 * members[0], 3 * members[-1] + 3)
        if sign > 0:
            weights = kernel_ref[taps[0] : taps[-1] + 1].reshape(-1, kernel_ref.shape[-1])
            part = jnp.dot(cells, weights, preferred_element_type=F32)
        else:
            weights = jnp.concatenate([kernel_ref[tap] for tap in taps], axis=1)
            part = lax.dot_general(
                cells, weights, (((1,), (1,)), ((), ())), preferred_element_type=F32
            )
        total = part if total is None else total + part
    return total


def window_of(rows):
    return [[shifted_columns(block) for block in row] for row in rows]


def block_rows(ref):
    return [[ref[row, frame] for frame in range(ref.shape[1])] for row in range(ref.shape[0])]


def silu_parts(pre_norm, gain):
    inverse = lax.rsqrt(jnp.mean(pre_norm * pre_norm, axis=-1, keepdims=True) + EPS)
    normed = pre_norm * inverse * gain
    return inverse, normed, 1.0 / (1.0 + jnp.exp(-normed))


def pre_norm_gradient(pre_norm, gain, upstream):
    inverse, normed, sigma = silu_parts(pre_norm, gain)
    scaled = gain * upstream * sigma * (1.0 + normed * (1.0 - sigma))
    mixed = jnp.mean(pre_norm * scaled, axis=-1, keepdims=True)
    return (inverse * scaled - pre_norm * inverse**3 * mixed).astype(BF16)


def at_last_tile():
    return lax.axis_index("tile") == lax.axis_size("tile") - 1


def first_rows(own, below_ref, first_frame, total):
    rows = own[0][0].shape[1]
    result = []
    for row in range(total):
        if row < rows:
            result.append([ref[frame, row] for ref, frame in own])
        else:
            result.append(
                [
                    below_ref[(first_frame + index) * rows + row - rows]
                    for index in range(len(own))
                ]
            )
    return result


def core_step(
    own_ref, earlier_ref, earliest_ref, later_ref, below_ref, above_ref, top_ref,
    first_kernel_ref, second_kernel_ref, gain_ref, next_ref, second_grad_ref, first_grad_ref,
    wide_store, next_store, store, wide_next, wide_grad, pre_ref,
):
    frames, rows, columns, _ = own_ref.shape
    first, last = lax.axis_index("tile") == 0, at_last_tile()
    own = [
        (ref, frame)
        for ref in (earliest_ref, earlier_ref, own_ref, later_ref)
        for frame in range(frames)
    ]
    deep = len(own)
    window = [[above_ref[frame * 2 + row] for frame in range(deep)] for row in range(2)]
    window += first_rows(own, below_ref, 0, 2 * rows)
    seams = {(rows, 2): last, (rows + 1, 0): last, (0, 2): first, (1, 0): first}
    store_columns(wide_store, window_of(window), (0, 1, 2), seams)
    middle = deep - 2
    for start in range(0, 2 * rows, 2):
        pre_norm = product(wide_store, seams, (start, start + 1), middle, 1, first_kernel_ref)
        _, normed, sigma = silu_parts(pre_norm, gain_ref[0:1])
        value = (normed * sigma).astype(BF16)
        for block in range(2 * middle):
            row, frame = start + block // middle, block % middle
            cells = slice(block * columns, (block + 1) * columns)
            wide_next[row, frame] = value[cells]
            if row >= 2 and frame < 2 * frames:
                next_ref[row - 2, frame] = value[cells]
            if 2 <= row < rows + 2 and frames <= frame < 2 * frames:
                place = ((row - 2) * frames + frame - frames) * columns
                pre_ref[place : place + columns] = pre_norm[cells]
    seams = {(rows - 1, 2): last, (rows, 0): last, (0, 0): first}
    store_columns(next_store, window_of(block_rows(wide_next)), (0, 1, 2), seams)
    spread = 2 * frames
    for start in range(0, rows + 2, 2):
        pre_norm = product(next_store, seams, (start, start + 1), spread, 1, second_kernel_ref)
        upstream = []
        for row in (start, start + 1):
            for frame in range(spread):
                if row >= rows:
                    upstream.append(below_ref[deep * rows + frame * 2 + row - rows])
                elif frame < frames:
                    upstream.append(top_ref[frame, row])
                else:
                    upstream.append(later_ref[frame - frames, rows + row])
        upstream = jnp.concatenate(upstream, axis=0).astype(F32)
        grad = pre_norm_gradient(pre_norm, gain_ref[1:2], upstream)
        for block in range(2 * spread):
            row, frame = start + block // spread, block % spread
            value = grad[block * columns : (block + 1) * columns]
            wide_grad[row, frame] = value
            if row >= 2 and frame < frames:
                second_grad_ref[row - 2, frame] = value
    seams = {(rows - 2, 2): last, (rows - 1, 0): last}
    store_columns(store, window_of(block_rows(wide_grad)), (2, 1, 0), seams)
    upstream = product(store, seams, range(rows), frames, -1, second_kernel_ref)
    upstream = upstream.astype(BF16).astype(F32)
    grad = pre_norm_gradient(pre_ref[...], gain_ref[0:1], upstream)
    first_grad_ref[...] = grad.reshape(first_grad_ref.shape)


def backward_rows(own_ref, later_ref, above_ref, frames):
    rows = own_ref.shape[0]
    result = []
    for row in range(2):
        result.append([above_ref[row, frame] for frame in range(2 * frames)])
    for row in range(rows):
        result.append(
            [own_ref[row, frame] for frame in range(frames)]
            + [later_ref[row, frame] for frame in range(frames)]
        )
    return result


def first_backward(own_ref, later_ref, above_ref, kernel_ref, out_ref, token_ref, store):
    rows, frames, columns, _ = own_ref.shape
    seams = {(0, 0): lax.axis_index("tile") == 0, (rows - 1, 2): at_last_tile()}
    window = window_of(backward_rows(own_ref, later_ref, above_ref, frames))
    store_columns(store, window, (2, 1, 0), seams)
    grad = product(store, seams, range(rows), frames, -1, kernel_ref).astype(BF16)
    for row in range(rows):
        for frame in range(frames):
            cell = (row * frames + frame) * columns
            out_ref[frame, row] = grad[cell : cell + columns]
    token_ref[...] = grad[: token_ref.shape[0]].astype(F32)


def split_gradient(store, seams, grad_ref, keep_ref, send_ref):
    chips, _, share, channels = keep_ref.shape
    rows, frames, _, _ = grad_ref.shape
    odd = lax.axis_index("tile") % 2 == 1
    grad = grad_ref[...].reshape(-1, channels)
    for index in range(9):
        blocks = lax.dot_general(
            side_by_side(store, seams, range(rows), frames, 1, index),
            grad,
            (((0,), (0,)), ((), ())),
            preferred_element_type=F32,
        )
        for across in range(3):
            block = blocks[across * channels : (across + 1) * channels]
            block = block.reshape(chips, 2, share, channels)
            even_part, odd_part = block[:, 0], block[:, 1]
            tap = 3 * index + across
            keep_ref[:, tap] = jnp.where(odd, odd_part, even_part).astype(BF16)
            send_ref[:, tap] = jnp.where(odd, even_part, odd_part).astype(BF16)


def second_kernel_gradient(next_ref, grad_ref, keep_ref, send_ref, store):
    rows = grad_ref.shape[0]
    last = at_last_tile()
    seams = {(rows - 3, 2): last, (rows - 2, 0): last}
    store_columns(store, window_of(block_rows(next_ref)), (0, 1, 2), seams)
    split_gradient(store, seams, grad_ref, keep_ref, send_ref)


def first_kernel_gradient(
    own_ref, earlier_ref, below_ref, grad_ref, keep_second, send_second, keep_ref, send_ref, store
):
    rows = grad_ref.shape[0]
    last = at_last_tile()
    seams = {(rows - 2, 2): last, (rows - 1, 0): last}
    frames = own_ref.shape[0]
    own = [(ref, frame) for ref in (earlier_ref, own_ref) for frame in range(frames)]
    window = window_of(first_rows(own, below_ref, frames, rows + 2))
    store_columns(store, window, (0, 1, 2), seams)
    keep_ref[:, TAPS:], send_ref[:, TAPS:] = keep_second[...], send_second[...]
    split_gradient(store, seams, grad_ref, keep_ref, send_ref)


def pack_inputs(
    own_ref, earlier_ref, earliest_ref, later_ref, top_ref, below_ref, above_ref
):
    frames, rows = own_ref.shape[:2]
    parts = (earliest_ref, earlier_ref, own_ref, later_ref)
    for index, part in enumerate(parts):
        for frame in range(frames):
            place = index * frames + frame
            below_ref[place * rows : (place + 1) * rows] = part[frame, :rows]
            above_ref[place * 2 : (place + 1) * 2] = part[frame, rows - 2 : rows]
    base = len(parts) * frames * rows
    for frame in range(frames):
        below_ref[base + frame * 2 : base + frame * 2 + 2] = top_ref[frame, :2]
        place = base + (frames + frame) * 2
        below_ref[place : place + 2] = later_ref[frame, rows : rows + 2]


def pack_rows(own_ref, later_ref, out_ref):
    frames, first = own_ref.shape[1], own_ref.shape[0] - out_ref.shape[0]
    out_ref[:, :frames] = own_ref[first:]
    out_ref[:, frames:] = later_ref[first:]


def add_pair(keep_ref, came_ref, out_ref):
    out_ref[...] = (keep_ref[...].astype(F32) + came_ref[...].astype(F32)).astype(BF16)


def sum_tiles(share, in_ref, token_ref, out_ref, rows_ref):
    del token_ref
    total = in_ref[0].astype(F32)
    for chip in range(1, in_ref.shape[0]):
        total = total + in_ref[chip].astype(F32)
    groups, width, lanes = out_ref.shape
    stride, taps = lanes // share, 2 * TAPS
    total = total.reshape(taps, share, -1)
    rows_ref[...] = jnp.zeros_like(rows_ref)
    for place in range(share):
        rows_ref[place * stride : place * stride + taps] = total[:, place]
    out_ref[...] = rows_ref[...].T.reshape(groups, width, lanes).astype(BF16)


def sum_frames(scale, in_ref, out_ref):
    total = in_ref[0].astype(F32)
    for group in range(1, in_ref.shape[0]):
        total = total + in_ref[group].astype(F32)
    share, _, taps = out_ref.shape
    stride = total.shape[1] // share
    for place in range(share):
        out_ref[place] = total[:, place * stride : place * stride + taps] * scale


def shape_of(*dims, dtype=BF16):
    return jax.ShapeDtypeStruct(dims, dtype)


def local(saved_codes, saved_scales, kernels, norm_gains, cotangent):
    frames, rows, columns, channels = saved_codes.shape
    tiles, groups = lax.axis_size("tile"), lax.axis_size("frame")
    cells = frames * rows * columns
    block = (columns, channels)

    def column_store(window_rows, window_frames):
        return (pltpu.VMEM((window_rows + 2, window_frames, columns, 3 * channels), BF16),)

    def next_frames(value, steps):
        return lax.ppermute(value, "frame", [(i, i + steps) for i in range(groups - steps)])

    def earlier_frames(value):
        return lax.ppermute(value, "frame", [(i + 1, i) for i in range(groups - 1)])

    def from_below(value):
        return lax.ppermute(value, "tile", [((i + 1) % tiles, i) for i in range(tiles)])

    def from_above(value):
        return lax.ppermute(value, "tile", [(i, (i + 1) % tiles) for i in range(tiles)])

    def partner(value):
        return lax.ppermute(value, "tile", [(i, i ^ 1) for i in range(tiles)])

    own_0 = (saved_codes.astype(F32) * saved_scales[..., None]).astype(BF16)
    earliest_0, earlier_0 = next_frames(own_0, 2), next_frames(own_0, 1)
    later = earlier_frames(jnp.concatenate([own_0, cotangent], axis=1))

    count = 4 * frames
    to_above, to_below = call(
        pack_inputs,
        (shape_of(count * rows + 4 * frames, *block), shape_of(2 * count, *block)),
        own_0,
        earlier_0,
        earliest_0,
        later,
        cotangent,
    )
    below, above = from_below(to_above), from_above(to_below)
    wide, deep = 2 * rows, 3 * frames
    grad_shape = shape_of(rows, frames, *block)
    next_1, grad_1, grad_0 = call(
        core_step,
        (shape_of(wide - 2, 2 * frames, *block), grad_shape, grad_shape),
        own_0,
        earlier_0,
        earliest_0,
        later,
        below,
        above,
        cotangent,
        kernels[0],
        kernels[1],
        norm_gains,
        scratch=column_store(wide + 4, 4 * frames)
        + column_store(wide + 1, deep)
        + column_store(rows + 2, 2 * frames)
        + (
            pltpu.VMEM((wide, deep, *block), BF16),
            pltpu.VMEM((rows + 2, 2 * frames, *block), BF16),
            pltpu.VMEM((cells, channels), F32),
        ),
    )

    share = channels // tiles
    part = shape_of(tiles // 2, TAPS, share, channels)
    both = shape_of(tiles // 2, 2 * TAPS, share, channels)
    mark = shape_of(8, channels, dtype=F32)

    def neighbours(grad):
        later = earlier_frames(grad)
        packed = call(pack_rows, shape_of(2, 2 * frames, *block), grad, later)
        return later, from_above(packed)

    keep_1, send_1 = call(
        second_kernel_gradient,
        (part, part),
        next_1,
        grad_1,
        scratch=column_store(wide - 2, 2 * frames),
    )
    keep, send = call(
        first_kernel_gradient,
        (both, both),
        own_0,
        earlier_0,
        below,
        grad_0,
        keep_1,
        send_1,
        scratch=column_store(rows + 2, 2 * frames),
    )
    full = shape_of(tiles // 2, 2 * TAPS * share, channels)
    came = partner(send).reshape(full.shape)
    paired = call(add_pair, full, keep.reshape(full.shape), came)
    by_core = [list(range(core, tiles, 2)) for core in range(2)]
    arrived = lax.all_to_all(paired, "tile", 0, 0, tiled=True, axis_index_groups=by_core)
    next_to = neighbours(grad_0)
    input_grad, token = call(
        first_backward,
        (shape_of(frames, rows, *block), mark),
        grad_0,
        *next_to,
        kernels[0],
        scratch=column_store(rows + 2, 2 * frames),
    )
    lanes = 64 * share
    by_frame = call(
        lambda *refs: sum_tiles(share, *refs),
        shape_of(groups, channels // groups, lanes),
        arrived,
        token,
        scratch=(pltpu.VMEM((lanes, channels), F32),),
    )
    spread = lax.all_to_all(by_frame, "frame", 0, 0, tiled=True)
    scale = 1.0 / math.sqrt(cells * tiles * groups)
    summed = call(
        lambda *refs: sum_frames(scale, *refs),
        shape_of(share, channels // groups, 2 * TAPS, dtype=F32),
        spread,
    )
    return (input_grad, jnp.transpose(summed, (2, 0, 1)))


def solution(mesh):
    in_specs = (
        P("frame", "tile", None, None),
        P("frame", "tile", None),
        P(),
        P(),
        P("frame", "tile", None, None),
    )
    out_specs = (P("frame", "tile", None, None), P(None, "tile", "frame"))

    return jax.shard_map(local, mesh=mesh, in_specs=in_specs, out_specs=out_specs, check_vma=False)
```

```python
import math

import jax
import jax.numpy as jnp
from jax import lax
from jax.experimental import pallas as pl
from jax.experimental.pallas import tpu as pltpu
from jax.sharding import PartitionSpec as P


EPS = 1e-06
TAPS = 27
F32 = jnp.float32
BF16 = jnp.bfloat16


def call(kernel, out_shape, *operands, scratch=()):
    return pl.pallas_call(
        kernel,
        out_shape=out_shape,
        scratch_shapes=list(scratch),
        compiler_params=pltpu.CompilerParams(vmem_limit_bytes=48 * 2**20),
    )(*operands)


def shifted_columns(block):
    shape = block.shape
    columns = shape[-2]
    flat = block.astype(F32).reshape(-1, shape[-1])
    column = lax.broadcasted_iota(jnp.int32, flat.shape, 0) % columns
    before = jnp.where(column == 0, 0.0, pltpu.roll(flat, 1, 0))
    after = jnp.where(column == columns - 1, 0.0, pltpu.roll(flat, flat.shape[0] - 1, 0))
    return before.astype(BF16).reshape(shape), block, after.astype(BF16).reshape(shape)


def store_columns(store, window, order, seams):
    for row, blocks in enumerate(window):
        for frame, triple in enumerate(blocks):
            store[row, frame] = jnp.concatenate([triple[across] for across in order], axis=1)
    for extra, ((row, offset), seam) in enumerate(seams.items()):
        for frame in range(store.shape[1]):
            source = store[row + offset, frame]
            store[len(window) + extra, frame] = jnp.where(seam, jnp.zeros_like(source), source)


def side_by_side(store, seams, rows, frames, sign, index):
    depth, down = divmod(index, 3)
    if sign < 0:
        depth, down = 2 - depth, 2 - down
    extra, total = list(seams), store.shape[0] - len(seams)
    pieces = []
    for row in rows:
        place = total + extra.index((row, down)) if (row, down) in seams else row + down
        pieces.append(store[place, depth : depth + frames].reshape(-1, store.shape[-1]))
    return jnp.concatenate(pieces, axis=0)


def product(store, seams, rows, frames, sign, kernel_ref):
    total = None
    for index in range(0, 9, 2):
        members = range(index, min(index + 2, 9))
        cells = jnp.concatenate(
            [side_by_side(store, seams, rows, frames, sign, member) for member in members], axis=1
        )
        taps = range(3 * members[0], 3 * members[-1] + 3)
        if sign > 0:
            weights = kernel_ref[taps[0] : taps[-1] + 1].reshape(-1, kernel_ref.shape[-1])
            part = jnp.dot(cells, weights, preferred_element_type=F32)
        else:
            weights = jnp.concatenate([kernel_ref[tap] for tap in taps], axis=1)
            part = lax.dot_general(
                cells, weights, (((1,), (1,)), ((), ())), preferred_element_type=F32
            )
        total = part if total is None else total + part
    return total


def window_of(rows):
    return [[shifted_columns(block) for block in row] for row in rows]


def block_rows(ref):
    return [[ref[row, frame] for frame in range(ref.shape[1])] for row in range(ref.shape[0])]


def silu_parts(pre_norm, gain):
    inverse = lax.rsqrt(jnp.mean(pre_norm * pre_norm, axis=-1, keepdims=True) + EPS)
    normed = pre_norm * inverse * gain
    return inverse, normed, 1.0 / (1.0 + jnp.exp(-normed))


def pre_norm_gradient(pre_norm, gain, upstream):
    inverse, normed, sigma = silu_parts(pre_norm, gain)
    scaled = gain * upstream * sigma * (1.0 + normed * (1.0 - sigma))
    mixed = jnp.mean(pre_norm * scaled, axis=-1, keepdims=True)
    return (inverse * scaled - pre_norm * inverse**3 * mixed).astype(BF16)


def at_last_tile():
    return lax.axis_index("tile") == lax.axis_size("tile") - 1


def first_rows(own, below_ref, first_frame, total):
    rows = own[0][0].shape[1]
    result = []
    for row in range(total):
        if row < rows:
            result.append([ref[frame, row] for ref, frame in own])
        else:
            result.append(
                [
                    below_ref[(first_frame + index) * rows + row - rows]
                    for index in range(len(own))
                ]
            )
    return result


def core_step(
    own_ref, earlier_ref, earliest_ref, later_ref, below_ref, above_ref, joined_ref,
    first_kernel_ref, second_kernel_ref, gain_ref, next_ref, second_grad_ref, first_grad_ref,
    wide_store, next_store, store, wide_next, wide_grad, pre_ref,
):
    frames, rows, columns, _ = own_ref.shape
    first, last = lax.axis_index("tile") == 0, at_last_tile()
    own = [
        (ref, frame)
        for ref in (earliest_ref, earlier_ref, own_ref, later_ref)
        for frame in range(frames)
    ]
    deep = len(own)
    window = [[above_ref[frame * 2 + row] for frame in range(deep)] for row in range(2)]
    window += first_rows(own, below_ref, 0, 2 * rows)
    seams = {(rows, 2): last, (rows + 1, 0): last, (0, 2): first, (1, 0): first}
    store_columns(wide_store, window_of(window), (0, 1, 2), seams)
    middle = deep - 2
    for start in range(0, 2 * rows, 2):
        pre_norm = product(wide_store, seams, (start, start + 1), middle, 1, first_kernel_ref)
        _, normed, sigma = silu_parts(pre_norm, gain_ref[0:1])
        value = (normed * sigma).astype(BF16)
        for block in range(2 * middle):
            row, frame = start + block // middle, block % middle
            cells = slice(block * columns, (block + 1) * columns)
            wide_next[row, frame] = value[cells]
            if row >= 2 and frame < 2 * frames:
                next_ref[row - 2, frame] = value[cells]
            if 2 <= row < rows + 2 and frames <= frame < 2 * frames:
                place = ((row - 2) * frames + frame - frames) * columns
                pre_ref[place : place + columns] = pre_norm[cells]
    seams = {(rows - 1, 2): last, (rows, 0): last, (0, 0): first}
    store_columns(next_store, window_of(block_rows(wide_next)), (0, 1, 2), seams)
    spread = 2 * frames
    for start in range(0, rows + 2, 2):
        pre_norm = product(next_store, seams, (start, start + 1), spread, 1, second_kernel_ref)
        upstream = []
        for row in (start, start + 1):
            for frame in range(spread):
                if row >= rows:
                    upstream.append(below_ref[deep * rows + frame * 2 + row - rows])
                elif frame < frames:
                    upstream.append(joined_ref[frame, rows + row])
                else:
                    upstream.append(later_ref[frame - frames, rows + row])
        upstream = jnp.concatenate(upstream, axis=0).astype(F32)
        grad = pre_norm_gradient(pre_norm, gain_ref[1:2], upstream)
        for block in range(2 * spread):
            row, frame = start + block // spread, block % spread
            value = grad[block * columns : (block + 1) * columns]
            wide_grad[row, frame] = value
            if row >= 2 and frame < frames:
                second_grad_ref[row - 2, frame] = value
    seams = {(rows - 2, 2): last, (rows - 1, 0): last}
    store_columns(store, window_of(block_rows(wide_grad)), (2, 1, 0), seams)
    upstream = product(store, seams, range(rows), frames, -1, second_kernel_ref)
    upstream = upstream.astype(BF16).astype(F32)
    grad = pre_norm_gradient(pre_ref[...], gain_ref[0:1], upstream)
    first_grad_ref[...] = grad.reshape(first_grad_ref.shape)


def backward_rows(own_ref, later_ref, above_ref, frames):
    rows = own_ref.shape[0]
    result = []
    for row in range(2):
        result.append([above_ref[row, frame] for frame in range(2 * frames)])
    for row in range(rows):
        result.append(
            [own_ref[row, frame] for frame in range(frames)]
            + [later_ref[row, frame] for frame in range(frames)]
        )
    return result


def first_backward(own_ref, later_ref, above_ref, kernel_ref, out_ref, token_ref, store):
    rows, frames, columns, _ = own_ref.shape
    seams = {(0, 0): lax.axis_index("tile") == 0, (rows - 1, 2): at_last_tile()}
    window = window_of(backward_rows(own_ref, later_ref, above_ref, frames))
    store_columns(store, window, (2, 1, 0), seams)
    grad = product(store, seams, range(rows), frames, -1, kernel_ref).astype(BF16)
    for row in range(rows):
        for frame in range(frames):
            cell = (row * frames + frame) * columns
            out_ref[frame, row] = grad[cell : cell + columns]
    token_ref[...] = grad[: token_ref.shape[0]].astype(F32)


def split_gradient(store, seams, grad_ref, keep_ref, send_ref):
    chips, _, share, channels = keep_ref.shape
    rows, frames, _, _ = grad_ref.shape
    odd = lax.axis_index("tile") % 2 == 1
    grad = grad_ref[...].reshape(-1, channels)
    for index in range(9):
        blocks = lax.dot_general(
            side_by_side(store, seams, range(rows), frames, 1, index),
            grad,
            (((0,), (0,)), ((), ())),
            preferred_element_type=F32,
        )
        for across in range(3):
            block = blocks[across * channels : (across + 1) * channels]
            block = block.reshape(chips, 2, share, channels)
            even_part, odd_part = block[:, 0], block[:, 1]
            tap = 3 * index + across
            keep_ref[:, tap] = jnp.where(odd, odd_part, even_part).astype(BF16)
            send_ref[:, tap] = jnp.where(odd, even_part, odd_part).astype(BF16)


def second_kernel_gradient(next_ref, grad_ref, keep_ref, send_ref, store):
    rows = grad_ref.shape[0]
    last = at_last_tile()
    seams = {(rows - 3, 2): last, (rows - 2, 0): last}
    store_columns(store, window_of(block_rows(next_ref)), (0, 1, 2), seams)
    split_gradient(store, seams, grad_ref, keep_ref, send_ref)


def first_kernel_gradient(
    own_ref, earlier_ref, below_ref, grad_ref, keep_second, send_second, keep_ref, send_ref, store
):
    rows = grad_ref.shape[0]
    last = at_last_tile()
    seams = {(rows - 2, 2): last, (rows - 1, 0): last}
    frames = own_ref.shape[0]
    own = [(ref, frame) for ref in (earlier_ref, own_ref) for frame in range(frames)]
    window = window_of(first_rows(own, below_ref, frames, rows + 2))
    store_columns(store, window, (0, 1, 2), seams)
    keep_ref[:, TAPS:], send_ref[:, TAPS:] = keep_second[...], send_second[...]
    split_gradient(store, seams, grad_ref, keep_ref, send_ref)


def pack_inputs(
    own_ref, earlier_ref, earliest_ref, later_ref, joined_ref, below_ref, above_ref
):
    frames, rows = own_ref.shape[:2]
    parts = (earliest_ref, earlier_ref, own_ref, later_ref)
    for index, part in enumerate(parts):
        for frame in range(frames):
            place = index * frames + frame
            below_ref[place * rows : (place + 1) * rows] = part[frame, :rows]
            above_ref[place * 2 : (place + 1) * 2] = part[frame, rows - 2 : rows]
    base = len(parts) * frames * rows
    for frame in range(frames):
        below_ref[base + frame * 2 : base + frame * 2 + 2] = joined_ref[frame, rows : rows + 2]
        place = base + (frames + frame) * 2
        below_ref[place : place + 2] = later_ref[frame, rows : rows + 2]


def pack_rows(own_ref, later_ref, out_ref):
    frames, first = own_ref.shape[1], own_ref.shape[0] - out_ref.shape[0]
    out_ref[:, :frames] = own_ref[first:]
    out_ref[:, frames:] = later_ref[first:]


def add_pair(keep_ref, came_ref, out_ref):
    out_ref[...] = (keep_ref[...].astype(F32) + came_ref[...].astype(F32)).astype(BF16)


def sum_tiles(share, in_ref, token_ref, out_ref, rows_ref):
    del token_ref
    total = in_ref[0].astype(F32)
    for chip in range(1, in_ref.shape[0]):
        total = total + in_ref[chip].astype(F32)
    groups, width, lanes = out_ref.shape
    stride, taps = lanes // share, 2 * TAPS
    total = total.reshape(taps, share, -1)
    rows_ref[...] = jnp.zeros_like(rows_ref)
    for place in range(share):
        rows_ref[place * stride : place * stride + taps] = total[:, place]
    out_ref[...] = rows_ref[...].T.reshape(groups, width, lanes).astype(BF16)


def sum_frames(scale, in_ref, out_ref):
    total = in_ref[0].astype(F32)
    for group in range(1, in_ref.shape[0]):
        total = total + in_ref[group].astype(F32)
    share, _, taps = out_ref.shape
    stride = total.shape[1] // share
    for place in range(share):
        out_ref[place] = total[:, place * stride : place * stride + taps] * scale


def shape_of(*dims, dtype=BF16):
    return jax.ShapeDtypeStruct(dims, dtype)


def local(saved_codes, saved_scales, kernels, norm_gains, cotangent):
    frames, rows, columns, channels = saved_codes.shape
    tiles, groups = lax.axis_size("tile"), lax.axis_size("frame")
    cells = frames * rows * columns
    block = (columns, channels)

    def column_store(window_rows, window_frames):
        return (pltpu.VMEM((window_rows + 2, window_frames, columns, 3 * channels), BF16),)

    def next_frames(value, steps):
        return lax.ppermute(value, "frame", [(i, i + steps) for i in range(groups - steps)])

    def earlier_frames(value):
        return lax.ppermute(value, "frame", [(i + 1, i) for i in range(groups - 1)])

    def from_below(value):
        return lax.ppermute(value, "tile", [((i + 1) % tiles, i) for i in range(tiles)])

    def from_above(value):
        return lax.ppermute(value, "tile", [(i, (i + 1) % tiles) for i in range(tiles)])

    def partner(value):
        return lax.ppermute(value, "tile", [(i, i ^ 1) for i in range(tiles)])

    own_0 = (saved_codes.astype(F32) * saved_scales[..., None]).astype(BF16)
    joined = jnp.concatenate([own_0, cotangent], axis=1)
    earliest_0 = next_frames(own_0, 2)
    earlier_0 = next_frames(own_0, 1)
    later = earlier_frames(joined)

    count = 4 * frames
    to_above, to_below = call(
        pack_inputs,
        (shape_of(count * rows + 4 * frames, *block), shape_of(2 * count, *block)),
        own_0,
        earlier_0,
        earliest_0,
        later,
        joined,
    )
    below, above = from_below(to_above), from_above(to_below)
    wide, deep = 2 * rows, 3 * frames
    grad_shape = shape_of(rows, frames, *block)
    next_1, grad_1, grad_0 = call(
        core_step,
        (shape_of(wide - 2, 2 * frames, *block), grad_shape, grad_shape),
        own_0,
        earlier_0,
        earliest_0,
        later,
        below,
        above,
        joined,
        kernels[0],
        kernels[1],
        norm_gains,
        scratch=column_store(wide + 4, 4 * frames)
        + column_store(wide + 1, deep)
        + column_store(rows + 2, 2 * frames)
        + (
            pltpu.VMEM((wide, deep, *block), BF16),
            pltpu.VMEM((rows + 2, 2 * frames, *block), BF16),
            pltpu.VMEM((cells, channels), F32),
        ),
    )

    share = channels // tiles
    part = shape_of(tiles // 2, TAPS, share, channels)
    both = shape_of(tiles // 2, 2 * TAPS, share, channels)
    mark = shape_of(8, channels, dtype=F32)

    def neighbours(grad):
        later = earlier_frames(grad)
        packed = call(pack_rows, shape_of(2, 2 * frames, *block), grad, later)
        return later, from_above(packed)

    keep_1, send_1 = call(
        second_kernel_gradient,
        (part, part),
        next_1,
        grad_1,
        scratch=column_store(wide - 2, 2 * frames),
    )
    keep, send = call(
        first_kernel_gradient,
        (both, both),
        own_0,
        earlier_0,
        below,
        grad_0,
        keep_1,
        send_1,
        scratch=column_store(rows + 2, 2 * frames),
    )
    full = shape_of(tiles // 2, 2 * TAPS * share, channels)
    came = partner(send).reshape(full.shape)
    paired = call(add_pair, full, keep.reshape(full.shape), came)
    by_core = [list(range(core, tiles, 2)) for core in range(2)]
    arrived = lax.all_to_all(paired, "tile", 0, 0, tiled=True, axis_index_groups=by_core)
    next_to = neighbours(grad_0)
    input_grad, token = call(
        first_backward,
        (shape_of(frames, rows, *block), mark),
        grad_0,
        *next_to,
        kernels[0],
        scratch=column_store(rows + 2, 2 * frames),
    )
    lanes = 64 * share
    by_frame = call(
        lambda *refs: sum_tiles(share, *refs),
        shape_of(groups, channels // groups, lanes),
        arrived,
        token,
        scratch=(pltpu.VMEM((lanes, channels), F32),),
    )
    spread = lax.all_to_all(by_frame, "frame", 0, 0, tiled=True)
    scale = 1.0 / math.sqrt(cells * tiles * groups)
    summed = call(
        lambda *refs: sum_frames(scale, *refs),
        shape_of(share, channels // groups, 2 * TAPS, dtype=F32),
        spread,
    )
    return (input_grad, jnp.transpose(summed, (2, 0, 1)))


def solution(mesh):
    in_specs = (
        P("frame", "tile", None, None),
        P("frame", "tile", None),
        P(),
        P(),
        P("frame", "tile", None, None),
    )
    out_specs = (P("frame", "tile", None, None), P(None, "tile", "frame"))

    return jax.shard_map(local, mesh=mesh, in_specs=in_specs, out_specs=out_specs, check_vma=False)
```
